128 devices in a mesh: batch: 32 (over z, x, core), cols: 4 (over y).
Axes of the slice: x: 4, y: 4, z: 4, core: 2. Of those that a mesh axis runs over, the one named last changes fastest.
Arguments:
- partial_query: float32 [32, 1024, 1024], P('batch', None, 'cols'), may hold values from -1.25 to 1.25
- partial_key: float32 [32, 1024, 1024], P('batch', None, 'cols'), may hold values from -1.25 to 1.25
- partial_value: float32 [32, 1024, 1024], P('batch', None, 'cols'), may hold values from -1.25 to 1.25
- partial_mixed: float32 [32, 1024, 1024], P('batch', 'cols'), may hold values from -1.25 to 1.25
- partial_norm: float32 [32, 1024], P('batch'), may hold values from -12 to 12
- partial_bias: float32 [32, 1024], P('batch'), may hold values from -12 to 12
- master_query: float32 [1024, 1024], P('batch', 'cols'), may hold values from -0.1875 to 0.1875
- master_key: float32 [1024, 1024], P('batch', 'cols'), may hold values from -0.1875 to 0.1875
- master_value: float32 [1024, 1024], P('batch', 'cols'), may hold values from -0.1875 to 0.1875
- master_mixed: float32 [1024, 1024], P('cols', 'batch'), may hold values from -0.1875 to 0.1875
- master_norm: float32 [1024], P('batch'), may hold values from 0.25 to 1.75
- master_bias: float32 [1024], P('batch'), may hold values from -3 to 3
Outputs:
- compute_query: bfloat16 [1024, 1024], P(None, 'cols')
- compute_key: bfloat16 [1024, 1024], P(None, 'cols')
- compute_value: bfloat16 [1024, 1024], P(None, 'cols')
- compute_mixed: bfloat16 [1024, 1024], P('cols')
- compute_norm: bfloat16 [1024], replicated
- compute_bias: bfloat16 [1024], replicated
- stepped_query: float32 [1024, 1024], P('batch', 'cols')
- stepped_key: float32 [1024, 1024], P('batch', 'cols')
- stepped_value: float32 [1024, 1024], P('batch', 'cols')
- stepped_mixed: float32 [1024, 1024], P('cols', 'batch')
- stepped_norm: float32 [1024], P('batch')
- stepped_bias: float32 [1024], P('batch')
The draws below stay inside these ranges and needn't reach their ends.
All inputs are finite; a program needn't handle non-finite values.
Results may differ from the reference program's by a relative error of at most 0.001.
Values may be sent and summed in bfloat16 or wider, within the bound.
A program may use at most 64 MiB of HBM per device.

```python
import jax
import jax.numpy as jnp

WIDTH = 1024
ATTN = 1024
REPLICAS = 32


def with_spikes(array, stream_key, source, target, blocks, factor):
    owner, partner = [(jnp.arange(array.shape[axis_at]) // (array.shape[axis_at] // blocks)).reshape([-1 if axis == axis_at else 1 for axis in range(array.ndim)]) for axis_at in (source, target)]
    chosen = jax.random.permutation(stream_key, blocks)[partner]
    strong = (owner == chosen) | (owner == (partner + blocks // 2) % blocks)
    return jnp.where(strong, factor * array, array)


def levels(rng, extent, cuts, smallest, top_value):
    def one(position, blocks):
        heights = jax.random.uniform(jax.random.fold_in(jax.random.fold_in(rng, 6), position), (blocks,), jnp.float32, smallest / len(cuts), top_value / len(cuts))
        return jnp.repeat(jnp.exp(heights), extent[position] // blocks).reshape((-1,) + (1,) * (len(extent) - position - 1))

    loudness = one(*cuts[0])
    for cut in cuts[1:]:
        loudness = loudness * one(*cut)
    return loudness


def gaussian(stream_key, extent, spread, limit, shards=(), dtype=jnp.bfloat16):
    loudness = levels(stream_key, extent, shards, -0.22, 0.18) if shards else 1.0
    drawn = jax.random.normal(stream_key, extent, jnp.float32) * spread * loudness
    return jnp.minimum(jnp.maximum(drawn, -limit), limit).astype(dtype)


def heavy_noise(stream_key, dims, deviation, reach, cuts, heavy, kind=jnp.bfloat16):
    drawn = deviation * jax.random.normal(stream_key, dims, jnp.float32)
    if cuts:
        drawn = drawn * levels(stream_key, dims, cuts, -0.22, 0.18)
    return jnp.clip(with_spikes(drawn, jax.random.fold_in(stream_key, 3), *heavy), -reach, reach).astype(kind)


def setup_inputs(seed: int = 0) -> dict:
    splits = jax.random.split(jax.random.key(seed), 13)
    partial_query = heavy_noise(splits[0], (REPLICAS, WIDTH, ATTN), 0.1, 1.25, ((0, 32), (2, 4)), (0, 1, 32, 2.75), jnp.float32)
    partial_key = heavy_noise(splits[1], (REPLICAS, WIDTH, ATTN), 0.1, 1.25, ((0, 32), (2, 4)), (0, 1, 32, 2.75), jnp.float32)
    partial_value = heavy_noise(splits[2], (REPLICAS, WIDTH, ATTN), 0.1, 1.25, ((0, 32), (2, 4)), (0, 1, 32, 2.75), jnp.float32)
    partial_mixed = heavy_noise(splits[3], (REPLICAS, ATTN, WIDTH), 0.1, 1.25, ((0, 32), (1, 4)), (0, 2, 32, 2.75), jnp.float32)
    partial_norm = heavy_noise(splits[4], (REPLICAS, WIDTH), 1.0, 12.0, ((0, 32),), (0, 1, 32, 2.75), jnp.float32)
    partial_bias = heavy_noise(splits[5], (REPLICAS, WIDTH), 1.0, 12.0, ((0, 32),), (0, 1, 32, 2.75), jnp.float32)
    master_query = gaussian(splits[6], (WIDTH, ATTN), WIDTH ** -0.5, 0.1875, ((0, 32), (1, 4)), jnp.float32)
    master_key = gaussian(splits[7], (WIDTH, ATTN), WIDTH ** -0.5, 0.1875, ((0, 32), (1, 4)), jnp.float32)
    master_value = gaussian(splits[8], (WIDTH, ATTN), WIDTH ** -0.5, 0.1875, ((0, 32), (1, 4)), jnp.float32)
    master_mixed = gaussian(splits[9], (ATTN, WIDTH), ATTN ** -0.5, 0.1875, ((0, 4), (1, 32)), jnp.float32)
    master_norm = jnp.clip(1.0 + 0.15 * jax.random.normal(splits[10], (WIDTH,), jnp.float32), 0.25, 1.75)
    master_bias = gaussian(splits[11], (WIDTH,), 0.5, 3.0, ((0, 32),), jnp.float32)
    return {"partial_query": partial_query, "partial_key": partial_key, "partial_value": partial_value, "partial_mixed": partial_mixed, "partial_norm": partial_norm, "partial_bias": partial_bias, "master_query": master_query, "master_key": master_key, "master_value": master_value, "master_mixed": master_mixed, "master_norm": master_norm, "master_bias": master_bias}


learn_rate = 0.4


def reference(partial_query, partial_key, partial_value, partial_mixed, partial_norm, partial_bias, master_query, master_key, master_value, master_mixed, master_norm, master_bias):
    mean_query = jnp.sum(partial_query.astype(jnp.float32), axis=0) * REPLICAS ** -0.5
    mean_key = jnp.sum(partial_key.astype(jnp.float32), axis=0) * REPLICAS ** -0.5
    mean_value = jnp.sum(partial_value.astype(jnp.float32), axis=0) * REPLICAS ** -0.5
    mean_mixed = jnp.sum(partial_mixed.astype(jnp.float32), axis=0) * REPLICAS ** -0.5
    mean_norm = jnp.sum(partial_norm.astype(jnp.float32), axis=0) * REPLICAS ** -0.5
    mean_bias = jnp.sum(partial_bias.astype(jnp.float32), axis=0) * REPLICAS ** -0.5
    stepped_query = master_query - learn_rate * mean_query
    stepped_key = master_key - learn_rate * mean_key
    stepped_value = master_value - learn_rate * mean_value
    stepped_mixed = master_mixed - learn_rate * mean_mixed
    stepped_norm = master_norm - learn_rate * mean_norm
    stepped_bias = master_bias - learn_rate * mean_bias
    compute_query = stepped_query.astype(jnp.bfloat16)
    compute_key = stepped_key.astype(jnp.bfloat16)
    compute_value = stepped_value.astype(jnp.bfloat16)
    compute_mixed = stepped_mixed.astype(jnp.bfloat16)
    compute_norm = stepped_norm.astype(jnp.bfloat16)
    compute_bias = stepped_bias.astype(jnp.bfloat16)
    return compute_query, compute_key, compute_value, compute_mixed, compute_norm, compute_bias, stepped_query, stepped_key, stepped_value, stepped_mixed, stepped_norm, stepped_bias
```

```python
import math

import jax
import jax.numpy as jnp
from jax import lax
from jax.experimental import pallas as pl
from jax.experimental.pallas import tpu as pltpu
from jax.sharding import PartitionSpec as P

MESH = pl.DeviceIdType.MESH
F32 = jnp.float32
BF16 = jnp.bfloat16

RATE = 0.4 * 32**-0.5

SPREAD = 21.0
STEPS = 4096.0
SHIFT = 125.0
PAIR_TOP = 2.6
FOUR_TOP = 10.4


def encoded(x, top):
    log = jnp.log(1.0 + jnp.abs(x) * (STEPS / top))
    v = jnp.exp2(log * (SPREAD / math.log(2.0)) - SHIFT)
    return jnp.where(x < 0, -v, v).astype(BF16)


def decoded(code, top):
    v = code.astype(F32)
    log = jnp.log(jnp.abs(v))
    size = (jnp.exp2(log * (1.0 / (SPREAD * math.log(2.0))) + SHIFT / SPREAD) - 1.0) * (top / STEPS)
    return jnp.where(v < 0, -size, size)


def kernel(
    pm, pq, pk, pv, pn, pb, mm, mq, mk, mv, mn, mb,
    cm, cq, ck, cv, cn, cb, sm, sq, sk, sv, sn, sb,
    raw, flat, pair, send1, recv1, send2, recv2, acc, gat, mast,
    nbuf, npair, nx, nz, nmast,
    load_sem, mload_sem, nload_sem, d_send, d_recv,
    s1s, s1r, s2s, s2r, g1s, g1r, g2s, g2r, fs, fr, ns, nr,
):
    b = lax.axis_index("batch")
    col = lax.axis_index("cols")
    z, x, core = b // 8, (b // 2) % 4, b % 2

    def at(z, x, core):
        return (z * 8 + x * 2 + core, col)

    def step(h, j):
        return ((z, (x + j) % 4), (x + j) % 4) if h == 0 else (((z + j) % 4, x), (z + j) % 4)

    def wait(ref, sem):
        pltpu.make_async_copy(ref, ref, sem).wait()

    loads = [pltpu.make_async_copy(pm, flat, load_sem.at[0])]
    for a, ref in ((1, pq), (2, pk), (3, pv)):
        loads.append(pltpu.make_async_copy(ref, raw.at[a], load_sem.at[a]))
    small = [
        pltpu.make_async_copy(pn, nbuf.at[0], nload_sem.at[0]),
        pltpu.make_async_copy(pb, nbuf.at[1], nload_sem.at[1]),
        pltpu.make_async_copy(mn, nmast.at[0], nload_sem.at[2]),
        pltpu.make_async_copy(mb, nmast.at[1], nload_sem.at[3]),
    ]
    masters = [pltpu.make_async_copy(ref, mast.at[a], mload_sem.at[a]) for a, ref in enumerate((mm, mq, mk, mv))]
    loads[0].start()
    for copy in small:
        copy.start()
    for copy in loads[1:]:
        copy.start()
    for copy in masters:
        copy.start()

    barrier = pltpu.get_barrier_semaphore()
    peers = [at(z, x, 1 - core)]
    for j in (1, 2, 3):
        peers += [at(*step(0, j)[0], core), at(*step(1, j)[0], core)]
    for peer in peers:
        pl.semaphore_signal(barrier, inc=1, device_id=peer, device_id_type=MESH)

    for copy in small:
        copy.wait()
    lanes = lax.broadcasted_iota(jnp.int32, (8, 128), 1)
    rows = lax.broadcasted_iota(jnp.int32, (8, 128), 0)
    mine = (rows * 4 + lanes // 32) == b
    for i in range(2):
        m = jnp.concatenate([nmast[i]] * 4, axis=1)
        nbuf[i] = jnp.where(mine, jnp.broadcast_to(m, (8, 128)), 0.0) - RATE * nbuf[i]

    loads[0].wait()
    raw[0] = flat[...].T.reshape(16, 2, 32, 256)

    pl.semaphore_wait(barrier, 7)

    sends = []

    def remote(src, dst, ssem, rsem, dev):
        copy = pltpu.make_async_remote_copy(
            src_ref=src, dst_ref=dst, send_sem=ssem, recv_sem=rsem, device_id=dev, device_id_type=MESH
        )
        copy.start()
        sends.append(copy)

    partner = at(z, x, 1 - core)
    remote(nbuf, npair, ns.at[0], nr.at[0], partner)
    for a in range(4):
        if a:
            loads[a].wait()
        remote(raw.at[a, :, 1 - core], pair.at[a], d_send.at[a], d_recv.at[a], partner)

    def pair_sum(a, zi, xi, h):
        i = zi * 4 + xi
        c = slice(128 * h, 128 * h + 128)
        return raw[a, i, core, :, c] + pair[a, i, :, c]

    def block(a, h, first, second):
        return pair_sum(a, second, first, h) if h == 0 else pair_sum(a, first, second, h)

    def e1(a):
        wait(pair.at[a], d_recv.at[a])
        for h in range(2):
            here = x if h == 0 else z
            for j in (2, 1, 3):
                dev, to = step(h, j)
                for k in range(4):
                    send1[a, h, j - 1, k] = encoded(block(a, h, to, k), PAIR_TOP)
                remote(send1.at[a, h, j - 1], recv1.at[a, h, j - 1], s1s.at[a, h, j - 1], s1r.at[a, h], at(*dev, core))
            for k in range(4):
                acc[a, h, k] = block(a, h, here, k)

    def r1(a):
        for h in range(2):
            wait(recv1.at[a, h], s1r.at[a, h])
            own = z if h == 0 else x

            def total(k):
                t = acc[a, h, k]
                for j in range(3):
                    t += decoded(recv1[a, h, j, k], PAIR_TOP)
                return t

            for j in (2, 1, 3):
                dev, to = step(1 - h, j)
                send2[a, h, j - 1] = encoded(total(to), FOUR_TOP)
                remote(send2.at[a, h, j - 1], recv2.at[a, h, j - 1], s2s.at[a, h, j - 1], s2r.at[a, h], at(*dev, core))
            acc[a, h, 0] = total(own)

    stepped = (sm, sq, sk, sv)

    def r2(a):
        masters[a].wait()
        for h in range(2):
            wait(recv2.at[a, h], s2r.at[a, h])
            t = acc[a, h, 0]
            for j in range(3):
                t += decoded(recv2[a, h, j], FOUR_TOP)
            c = slice(128 * h, 128 * h + 128)
            new = mast[a, :, c] - RATE * t
            stepped[a][:, c] = new
            first, second = (x, z) if h == 0 else (z, x)
            own = gat.at[a, h, core, first, second]
            gat[a, h, core, first, second] = new.astype(BF16)
            for j in (2, 1, 3):
                dev, _ = step(1 - h, j)
                remote(own, own, g1s.at[a, h, j - 1], g1r.at[a, h], at(*dev, core))

    def g1(a):
        for h in range(2):
            first = x if h == 0 else z
            row = gat.at[a, h, core, first]
            wait(gat.at[a, h, core, 0, pl.ds(0, 3)], g1r.at[a, h])
            for j in (2, 1, 3):
                dev, _ = step(h, j)
                remote(row, row, g2s.at[a, h, j - 1], g2r.at[a, h, j - 1], at(*dev, core))
            remote(row, row, fs.at[a, h, 3], fr.at[a, h], partner)

    def g2(a):
        for h in range(2):
            for j in (1, 3, 2):
                first = ((x if h == 0 else z) - j + 4) % 4
                row = gat.at[a, h, core, first]
                wait(row, g2r.at[a, h, j - 1])
                remote(row, row, fs.at[a, h, j - 1], fr.at[a, h], partner)

    outs = (cm, cq, ck, cv)

    def f(a):
        for h in range(2):
            wait(gat.at[a, h, 0], fr.at[a, h])
        for h in range(2):
            c = slice(128 * h, 128 * h + 128)
            order = (1, 2, 0, 3, 4) if h == 0 else (0, 2, 1, 3, 4)
            if a:
                for zi in range(4):
                    for xi in range(4):
                        for k in range(2):
                            first, second = (xi, zi) if h == 0 else (zi, xi)
                            outs[a][zi, xi, k, :, c] = gat[a, h, k, first, second]
            else:
                for zi in range(4):
                    for xi in range(0, 4, 2):
                        parts = []
                        for xj in (xi, xi + 1):
                            for k in range(2):
                                first, second = (xj, zi) if h == 0 else (zi, xj)
                                parts.append(gat[a, h, k, first, second])
                        at_lane = (zi * 4 + xi) * 64
                        outs[a][c, at_lane : at_lane + 128] = jnp.concatenate(parts, axis=0).T

    def n1():
        wait(npair, nr.at[0])
        nx[x] = nbuf[...] + npair[...]
        for j in (2, 1, 3):
            dev, _ = step(0, j)
            remote(nx.at[x], nx.at[x], ns.at[j], nr.at[1], at(*dev, core))

    def n2():
        wait(nx.at[pl.ds(0, 3)], nr.at[1])
        nz[z] = ((nx[0] + nx[1]) + nx[2]) + nx[3]
        for j in (2, 1, 3):
            dev, _ = step(1, j)
            remote(nz.at[z], nz.at[z], ns.at[3 + j], nr.at[2], at(*dev, core))

    def n3():
        wait(nz.at[pl.ds(0, 3)], nr.at[2])
        new = ((nz[0] + nz[1]) + nz[2]) + nz[3]
        cn[...] = new[0].astype(BF16)
        cb[...] = new[1].astype(BF16)
        place = jnp.sum(jnp.where(mine[None], new, 0.0), axis=1)
        slot = ((place[:, 0:32] + place[:, 32:64]) + place[:, 64:96]) + place[:, 96:128]
        sn[...] = slot[0:1]
        sb[...] = slot[1:2]

    for t in range(9):
        if t == 1:
            n1()
        if t == 2:
            n2()
        if t == 3:
            n3()
        for stage, lag in ((e1, 0), (r1, 1), (r2, 2), (g1, 3), (g2, 4), (f, 5)):
            if 0 <= t - lag < 4:
                stage(t - lag)

    for copy in sends:
        copy.wait_send()


def per_device(pq, pk, pv, pm, pn, pb, mq, mk, mv, mm, mn, mb):
    blocks = (16, 2, 32, 256)
    hbm = pl.BlockSpec(memory_space=pl.ANY)
    vmem = pl.BlockSpec(memory_space=pltpu.VMEM)
    dma = pltpu.SemaphoreType.DMA
    gathered = jax.ShapeDtypeStruct((4, 4, 2, 32, 256), BF16)
    share = jax.ShapeDtypeStruct((32, 256), F32)
    small = jax.ShapeDtypeStruct((8, 128), BF16)
    slot = jax.ShapeDtypeStruct((1, 32), F32)
    out = pl.pallas_call(
        kernel,
        out_shape=(jax.ShapeDtypeStruct((256, 1024), BF16), gathered, gathered, gathered, small, small)
        + (share,) * 4
        + (slot,) * 2,
        in_specs=[hbm] * 12,
        out_specs=(vmem,) * 12,
        scratch_shapes=[
            pltpu.VMEM((4, *blocks), F32),
            pltpu.VMEM((256, 1024), F32),
            pltpu.VMEM((4, 16, 32, 256), F32),
            pltpu.VMEM((4, 2, 3, 4, 32, 128), BF16),
            pltpu.VMEM((4, 2, 3, 4, 32, 128), BF16),
            pltpu.VMEM((4, 2, 3, 32, 128), BF16),
            pltpu.VMEM((4, 2, 3, 32, 128), BF16),
            pltpu.VMEM((4, 2, 4, 32, 128), F32),
            pltpu.VMEM((4, 2, 2, 4, 4, 32, 128), BF16),
            pltpu.VMEM((4, 32, 256), F32),
            pltpu.VMEM((2, 8, 128), F32),
            pltpu.VMEM((2, 8, 128), F32),
            pltpu.VMEM((4, 2, 8, 128), F32),
            pltpu.VMEM((4, 2, 8, 128), F32),
            pltpu.VMEM((2, 1, 32), F32),
            dma((4,)),
            dma((4,)),
            dma((4,)),
            dma((4,)),
            dma((4,)),
            dma((4, 2, 3)),
            dma((4, 2)),
            dma((4, 2, 3)),
            dma((4, 2)),
            dma((4, 2, 3)),
            dma((4, 2)),
            dma((4, 2, 3)),
            dma((4, 2, 3)),
            dma((4, 2, 4)),
            dma((4, 2)),
            dma((7,)),
            dma((3,)),
        ],
        compiler_params=pltpu.CompilerParams(collective_id=0, has_side_effects=True, vmem_limit_bytes=60 * 2**20),
        name="step",
    )(
        pm[0], pq.reshape(blocks), pk.reshape(blocks), pv.reshape(blocks), pn.reshape(8, 128), pb.reshape(8, 128),
        mm.T, mq, mk, mv, mn.reshape(1, 32), mb.reshape(1, 32),
    )
    cm, cq, ck, cv, cn, cb, sm, sq, sk, sv, sn, sb = out
    whole = (1024, 256)
    return (
        cq.reshape(whole), ck.reshape(whole), cv.reshape(whole), cm, cn.reshape(1024), cb.reshape(1024),
        sq, sk, sv, sm.T, sn.reshape(32), sb.reshape(32),
    )


def solution(mesh):
    in_specs = (
        P("batch", None, "cols"),
        P("batch", None, "cols"),
        P("batch", None, "cols"),
        P("batch", "cols", None),
        P("batch", None),
        P("batch", None),
        P("batch", "cols"),
        P("batch", "cols"),
        P("batch", "cols"),
        P("cols", "batch"),
        P("batch"),
        P("batch"),
    )
    out_specs = (
        P(None, "cols"),
        P(None, "cols"),
        P(None, "cols"),
        P("cols", None),
        P(),
        P(),
        P("batch", "cols"),
        P("batch", "cols"),
        P("batch", "cols"),
        P("cols", "batch"),
        P("batch"),
        P("batch"),
    )
    return jax.shard_map(per_device, mesh=mesh, in_specs=in_specs, out_specs=out_specs, check_vma=False)
```

```python
import math

import jax
import jax.numpy as jnp
from jax import lax
from jax.experimental import pallas as pl
from jax.experimental.pallas import tpu as pltpu
from jax.sharding import PartitionSpec as P

MESH = pl.DeviceIdType.MESH
F32 = jnp.float32
BF16 = jnp.bfloat16

RATE = 0.4 * 32**-0.5

SPREAD = 21.0
STEPS = 4096.0
SHIFT = 125.0
PAIR_TOP = 2.6
FOUR_TOP = 10.4


def encoded(x, top):
    log = jnp.log(1.0 + jnp.abs(x) * (STEPS / top))
    v = jnp.exp2(log * (SPREAD / math.log(2.0)) - SHIFT)
    return jnp.where(x < 0, -v, v).astype(BF16)


def decoded(code, top):
    v = code.astype(F32)
    log = jnp.log(jnp.abs(v))
    size = (jnp.exp2(log * (1.0 / (SPREAD * math.log(2.0))) + SHIFT / SPREAD) - 1.0) * (top / STEPS)
    return jnp.where(v < 0, -size, size)


def kernel(
    pm, pq, pk, pv, pn, pb, mm, mq, mk, mv, mn, mb,
    cm, cq, ck, cv, cn, cb, sm, sq, sk, sv, sn, sb,
    raw, flat, pair, send1, recv1, send2, recv2, acc, gat, mast,
    nbuf, npair, nx, nz, nmast,
    load_sem, mload_sem, nload_sem, d_send, d_recv,
    s1s, s1r, s2s, s2r, g1s, g1r, g2s, g2r, fs, fr, ns, nr,
):
    b = lax.axis_index("batch")
    col = lax.axis_index("cols")
    z, x, core = b // 8, (b // 2) % 4, b % 2

    def at(z, x, core):
        return (z * 8 + x * 2 + core, col)

    def step(h, j):
        return ((z, (x + j) % 4), (x + j) % 4) if h == 0 else (((z + j) % 4, x), (z + j) % 4)

    def wait(ref, sem):
        pltpu.make_async_copy(ref, ref, sem).wait()

    loads = [pltpu.make_async_copy(pm, flat, load_sem.at[0])]
    for a, ref in ((1, pq), (2, pk), (3, pv)):
        loads.append(pltpu.make_async_copy(ref, raw.at[a], load_sem.at[a]))
    small = [
        pltpu.make_async_copy(pn, nbuf.at[0], nload_sem.at[0]),
        pltpu.make_async_copy(pb, nbuf.at[1], nload_sem.at[1]),
        pltpu.make_async_copy(mn, nmast.at[0], nload_sem.at[2]),
        pltpu.make_async_copy(mb, nmast.at[1], nload_sem.at[3]),
    ]
    masters = [pltpu.make_async_copy(ref, mast.at[a], mload_sem.at[a]) for a, ref in enumerate((mm, mq, mk, mv))]
    loads[0].start()
    for copy in small:
        copy.start()
    for copy in loads[1:]:
        copy.start()
    for copy in masters:
        copy.start()

    barrier = pltpu.get_barrier_semaphore()
    peers = [at(z, x, 1 - core)]
    for j in (1, 2, 3):
        peers += [at(*step(0, j)[0], core), at(*step(1, j)[0], core)]
    for peer in peers:
        pl.semaphore_signal(barrier, inc=1, device_id=peer, device_id_type=MESH)

    for copy in small:
        copy.wait()
    lanes = lax.broadcasted_iota(jnp.int32, (8, 128), 1)
    rows = lax.broadcasted_iota(jnp.int32, (8, 128), 0)
    mine = (rows * 4 + lanes // 32) == b
    for i in range(2):
        m = jnp.concatenate([nmast[i]] * 4, axis=1)
        nbuf[i] = jnp.where(mine, jnp.broadcast_to(m, (8, 128)), 0.0) - RATE * nbuf[i]

    loads[0].wait()
    raw[0] = flat[...].T.reshape(16, 2, 32, 256)

    pl.semaphore_wait(barrier, 7)

    sends = []

    def remote(src, dst, ssem, rsem, dev):
        copy = pltpu.make_async_remote_copy(
            src_ref=src, dst_ref=dst, send_sem=ssem, recv_sem=rsem, device_id=dev, device_id_type=MESH
        )
        copy.start()
        sends.append(copy)

    partner = at(z, x, 1 - core)
    remote(nbuf, npair, ns.at[0], nr.at[0], partner)
    for a in range(4):
        if a:
            loads[a].wait()
        remote(raw.at[a, :, 1 - core], pair.at[a], d_send.at[a], d_recv.at[a], partner)

    def pair_sum(a, zi, xi, h):
        i = zi * 4 + xi
        c = slice(128 * h, 128 * h + 128)
        return raw[a, i, core, :, c] + pair[a, i, :, c]

    def block(a, h, first, second):
        return pair_sum(a, second, first, h) if h == 0 else pair_sum(a, first, second, h)

    def e1(a):
        wait(pair.at[a], d_recv.at[a])
        for h in range(2):
            here = x if h == 0 else z
            for j in (2, 1, 3):
                dev, to = step(h, j)
                for k in range(4):
                    send1[a, h, j - 1, k] = encoded(block(a, h, to, k), PAIR_TOP)
                remote(send1.at[a, h, j - 1], recv1.at[a, h, j - 1], s1s.at[a, h, j - 1], s1r.at[a, h], at(*dev, core))
            for k in range(4):
                acc[a, h, k] = block(a, h, here, k)

    def r1(a):
        for h in range(2):
            wait(recv1.at[a, h], s1r.at[a, h])
            own = z if h == 0 else x

            def total(k):
                t = acc[a, h, k]
                for j in range(3):
                    t += decoded(recv1[a, h, j, k], PAIR_TOP)
                return t

            for j in (2, 1, 3):
                dev, to = step(1 - h, j)
                send2[a, h, j - 1] = encoded(total(to), FOUR_TOP)
                remote(send2.at[a, h, j - 1], recv2.at[a, h, j - 1], s2s.at[a, h, j - 1], s2r.at[a, h], at(*dev, core))
            acc[a, h, 0] = total(own)

    stepped = (sm, sq, sk, sv)

    def r2(a):
        masters[a].wait()
        for h in range(2):
            wait(recv2.at[a, h], s2r.at[a, h])
            t = acc[a, h, 0]
            for j in range(3):
                t += decoded(recv2[a, h, j], FOUR_TOP)
            c = slice(128 * h, 128 * h + 128)
            new = mast[a, :, c] - RATE * t
            stepped[a][:, c] = new
            first, second = (x, z) if h == 0 else (z, x)
            own = gat.at[a, h, core, first, second]
            gat[a, h, core, first, second] = new.astype(BF16)
            for j in (2, 1, 3):
                dev, _ = step(1 - h, j)
                remote(own, own, g1s.at[a, h, j - 1], g1r.at[a, h], at(*dev, core))

    def g1(a):
        for h in range(2):
            first = x if h == 0 else z
            row = gat.at[a, h, core, first]
            wait(gat.at[a, h, core, 0, pl.ds(0, 3)], g1r.at[a, h])
            for j in (2, 1, 3):
                dev, _ = step(h, j)
                remote(row, row, g2s.at[a, h, j - 1], g2r.at[a, h, j - 1], at(*dev, core))
            remote(row, row, fs.at[a, h, 3], fr.at[a, h], partner)

    def g2(a):
        for h in range(2):
            for j in (1, 3, 2):
                first = ((x if h == 0 else z) - j + 4) % 4
                row = gat.at[a, h, core, first]
                wait(row, g2r.at[a, h, j - 1])
                remote(row, row, fs.at[a, h, j - 1], fr.at[a, h], partner)

    outs = (cm, cq, ck, cv)

    def f(a):
        for h in range(2):
            wait(gat.at[a, h, 0], fr.at[a, h])
        for h in range(2):
            c = slice(128 * h, 128 * h + 128)
            order = (1, 2, 0, 3, 4) if h == 0 else (0, 2, 1, 3, 4)
            if a:
                for zi in range(4):
                    for xi in range(4):
                        for k in range(2):
                            first, second = (xi, zi) if h == 0 else (zi, xi)
                            outs[a][zi, xi, k, :, c] = gat[a, h, k, first, second]
            else:
                for zi in range(4):
                    for xi in range(0, 4, 2):
                        parts = []
                        for xj in (xi, xi + 1):
                            for k in range(2):
                                first, second = (xj, zi) if h == 0 else (zi, xj)
                                parts.append(gat[a, h, k, first, second])
                        at_lane = (zi * 4 + xi) * 64
                        outs[a][c, at_lane : at_lane + 128] = jnp.concatenate(parts, axis=0).T

    def n1():
        wait(npair, nr.at[0])
        nx[x] = nbuf[...] + npair[...]
        for j in (2, 1, 3):
            dev, _ = step(0, j)
            remote(nx.at[x], nx.at[x], ns.at[j], nr.at[1], at(*dev, core))

    def n2():
        wait(nx.at[pl.ds(0, 3)], nr.at[1])
        nz[z] = ((nx[0] + nx[1]) + nx[2]) + nx[3]
        for j in (2, 1, 3):
            dev, _ = step(1, j)
            remote(nz.at[z], nz.at[z], ns.at[3 + j], nr.at[2], at(*dev, core))

    def n3():
        wait(nz.at[pl.ds(0, 3)], nr.at[2])
        new = ((nz[0] + nz[1]) + nz[2]) + nz[3]
        cn[...] = new[0].astype(BF16)
        cb[...] = new[1].astype(BF16)
        place = jnp.sum(jnp.where(mine[None], new, 0.0), axis=1)
        slot = ((place[:, 0:32] + place[:, 32:64]) + place[:, 64:96]) + place[:, 96:128]
        sn[...] = slot[0:1]
        sb[...] = slot[1:2]

    for t in range(9):
        if t == 1:
            n1()
        if t == 2:
            n2()
        if t == 3:
            n3()
        for stage, lag in ((e1, 0), (r1, 1), (r2, 2), (g1, 3), (g2, 4), (f, 5)):
            if 0 <= t - lag < 4:
                stage(t - lag)

    for copy in sends:
        copy.wait_send()


def placed(*refs):
    sems = refs[24]
    copies = [pltpu.make_async_copy(refs[i], refs[12 + i], sems.at[i]) for i in range(12)]
    for copy in copies:
        copy.start()
    for copy in copies:
        copy.wait()


def per_device(pq, pk, pv, pm, pn, pb, mq, mk, mv, mm, mn, mb):
    blocks = (16, 2, 32, 256)
    hbm = pl.BlockSpec(memory_space=pl.ANY)
    vmem = pl.BlockSpec(memory_space=pltpu.VMEM)
    dma = pltpu.SemaphoreType.DMA
    gathered = jax.ShapeDtypeStruct((4, 4, 2, 32, 256), BF16)
    share = jax.ShapeDtypeStruct((32, 256), F32)
    small = jax.ShapeDtypeStruct((8, 128), BF16)
    slot = jax.ShapeDtypeStruct((1, 32), F32)
    shapes = (jax.ShapeDtypeStruct((256, 1024), BF16), gathered, gathered, gathered, small, small)
    shapes += (share,) * 4 + (slot,) * 2
    out = pl.pallas_call(
        kernel,
        out_shape=tuple(pltpu.VMEM(o.shape, o.dtype) for o in shapes),
        in_specs=[hbm] * 12,
        out_specs=(vmem,) * 12,
        scratch_shapes=[
            pltpu.VMEM((4, *blocks), F32),
            pltpu.VMEM((256, 1024), F32),
            pltpu.VMEM((4, 16, 32, 256), F32),
            pltpu.VMEM((4, 2, 3, 4, 32, 128), BF16),
            pltpu.VMEM((4, 2, 3, 4, 32, 128), BF16),
            pltpu.VMEM((4, 2, 3, 32, 128), BF16),
            pltpu.VMEM((4, 2, 3, 32, 128), BF16),
            pltpu.VMEM((4, 2, 4, 32, 128), F32),
            pltpu.VMEM((4, 2, 2, 4, 4, 32, 128), BF16),
            pltpu.VMEM((4, 32, 256), F32),
            pltpu.VMEM((2, 8, 128), F32),
            pltpu.VMEM((2, 8, 128), F32),
            pltpu.VMEM((4, 2, 8, 128), F32),
            pltpu.VMEM((4, 2, 8, 128), F32),
            pltpu.VMEM((2, 1, 32), F32),
            dma((4,)),
            dma((4,)),
            dma((4,)),
            dma((4,)),
            dma((4,)),
            dma((4, 2, 3)),
            dma((4, 2)),
            dma((4, 2, 3)),
            dma((4, 2)),
            dma((4, 2, 3)),
            dma((4, 2)),
            dma((4, 2, 3)),
            dma((4, 2, 3)),
            dma((4, 2, 4)),
            dma((4, 2)),
            dma((7,)),
            dma((3,)),
        ],
        compiler_params=pltpu.CompilerParams(collective_id=0, has_side_effects=True, vmem_limit_bytes=60 * 2**20),
        name="step",
    )(
        pm[0], pq.reshape(blocks), pk.reshape(blocks), pv.reshape(blocks), pn.reshape(8, 128), pb.reshape(8, 128),
        mm.T, mq, mk, mv, mn.reshape(1, 32), mb.reshape(1, 32),
    )
    cm, cq, ck, cv, cn, cb, sm, sq, sk, sv, sn, sb = pl.pallas_call(
        placed,
        out_shape=shapes,
        in_specs=[vmem] * 12,
        out_specs=(hbm,) * 12,
        scratch_shapes=[dma((12,))],
        name="placed",
    )(*[pltpu.with_memory_space_constraint(o, pltpu.VMEM) for o in out])
    whole = (1024, 256)
    return (
        cq.reshape(whole), ck.reshape(whole), cv.reshape(whole), cm, cn.reshape(1024), cb.reshape(1024),
        sq, sk, sv, sm.T, sn.reshape(32), sb.reshape(32),
    )


def solution(mesh):
    in_specs = (
        P("batch", None, "cols"),
        P("batch", None, "cols"),
        P("batch", None, "cols"),
        P("batch", "cols", None),
        P("batch", None),
        P("batch", None),
        P("batch", "cols"),
        P("batch", "cols"),
        P("batch", "cols"),
        P("cols", "batch"),
        P("batch"),
        P("batch"),
    )
    out_specs = (
        P(None, "cols"),
        P(None, "cols"),
        P(None, "cols"),
        P("cols", None),
        P(),
        P(),
        P("batch", "cols"),
        P("batch", "cols"),
        P("batch", "cols"),
        P("cols", "batch"),
        P("batch"),
        P("batch"),
    )
    return jax.shard_map(per_device, mesh=mesh, in_specs=in_specs, out_specs=out_specs, check_vma=False)
```

```python
import math

import jax
import jax.numpy as jnp
from jax import lax
from jax.experimental import pallas as pl
from jax.experimental.pallas import tpu as pltpu
from jax.sharding import PartitionSpec as P

MESH = pl.DeviceIdType.MESH
F32 = jnp.float32
BF16 = jnp.bfloat16

RATE = 0.4 * 32**-0.5

SPREAD = 21.0
STEPS = 4096.0
SHIFT = 125.0
PAIR_TOP = 2.6
ORDER = (2, 1, 3, 0)
BACK = (1, 3, 2)
FOUR_TOP = 10.4


def encoded(x, top):
    log = jnp.log(1.0 + jnp.abs(x) * (STEPS / top))
    v = jnp.exp2(log * (SPREAD / math.log(2.0)) - SHIFT)
    return jnp.where(x < 0, -v, v).astype(BF16)


def decoded(code, top):
    v = code.astype(F32)
    log = jnp.log(jnp.abs(v))
    size = (jnp.exp2(log * (1.0 / (SPREAD * math.log(2.0))) + SHIFT / SPREAD) - 1.0) * (top / STEPS)
    return jnp.where(v < 0, -size, size)


def kernel(
    pm, pq, pk, pv, pn, pb, mm, mq, mk, mv, mn, mb,
    cm, cq, ck, cv, cn, cb, sm, sq, sk, sv, sn, sb,
    raw, flat, pair, send1, recv1, send2, recv2, acc, gat, mast,
    nbuf, npair, nx, nz, nmast,
    load_sem, mload_sem, nload_sem, d_recv, s1r, s2r, g1r, g2r, fr, sent, ns, nr,
):
    b = lax.axis_index("batch")
    col = lax.axis_index("cols")
    z, x, core = b // 8, (b // 2) % 4, b % 2
    first, second = (x, z), (z, x)

    def at(z, x, core):
        return (z * 8 + x * 2 + core, col)

    def ahead(axis, j):
        return at(z, (x + j) % 4, core) if axis == 0 else at((z + j) % 4, x, core)

    def wait(ref, sem):
        pltpu.make_async_copy(ref, ref, sem).wait()

    def remote(src, dst, ssem, rsem, dev):
        pltpu.make_async_remote_copy(
            src_ref=src, dst_ref=dst, send_sem=ssem, recv_sem=rsem, device_id=dev, device_id_type=MESH
        ).start()

    def lanes_of(h):
        return slice(128 * h, 128 * h + 128)

    barrier = pltpu.get_barrier_semaphore()
    partner = at(z, x, 1 - core)
    for peer in [partner] + [ahead(axis, j) for j in (2, 1, 3) for axis in (0, 1)]:
        pl.semaphore_signal(barrier, inc=1, device_id=peer, device_id_type=MESH)

    turned = pltpu.make_async_copy(pm, flat, load_sem.at[0])
    loads = {a: pltpu.make_async_copy(ref, raw.at[a], load_sem.at[a]) for a, ref in ((1, pq), (2, pk), (3, pv))}
    small = [
        pltpu.make_async_copy(pn, nbuf.at[0], nload_sem.at[0]),
        pltpu.make_async_copy(pb, nbuf.at[1], nload_sem.at[1]),
        pltpu.make_async_copy(mn, nmast.at[0], nload_sem.at[2]),
        pltpu.make_async_copy(mb, nmast.at[1], nload_sem.at[3]),
    ]
    masters = [pltpu.make_async_copy(ref, mast.at[a], mload_sem.at[a]) for a, ref in enumerate((mm, mq, mk, mv))]
    for copy in (turned, *small, loads[1], loads[2], loads[3], *masters):
        copy.start()

    for copy in small:
        copy.wait()
    lanes = lax.broadcasted_iota(jnp.int32, (8, 128), 1)
    rows = lax.broadcasted_iota(jnp.int32, (8, 128), 0)
    mine = (rows * 4 + lanes // 32) == b
    for i in range(2):
        m = jnp.concatenate([nmast[i]] * 4, axis=1)
        nbuf[i] = jnp.where(mine, jnp.broadcast_to(m, (8, 128)), 0.0) - RATE * nbuf[i]

    def piece(a_ref, h, k, core):
        return a_ref.at[:, k, :, core, :, lanes_of(h)] if h == 0 else a_ref.at[:, :, k, core, :, lanes_of(h)]

    turned.wait()
    raw[0] = flat[...].T.reshape(4, 4, 2, 32, 256)
    for a in (1, 2, 3):
        loads[a].wait()
    pl.semaphore_wait(barrier, 7)
    for r in ORDER:
        for h in range(2):
            k = (second[h] + r) % 4
            remote(piece(raw, h, k, 1 - core), pair.at[h, k], sent.at[0], d_recv.at[h, r], partner)
        if r == 1:
            remote(nbuf, npair, ns.at[0], nr.at[0], partner)

    def block(a, h, f, k):
        zi, xi = (k, f) if h == 0 else (f, k)
        return raw[a, zi, xi, core, :, lanes_of(h)] + pair[h, k, a, f]

    def e1(h, r):
        k = (second[h] + r) % 4
        wait(pair.at[h, k], d_recv.at[h, r])
        for j in (2, 1, 3):
            for a in range(4):
                send1[h, r, j - 1, a] = encoded(block(a, h, (first[h] + j) % 4, k), PAIR_TOP)
            remote(send1.at[h, r, j - 1], recv1.at[h, r, j - 1], sent.at[1], s1r.at[h, r], ahead(h, j))

    def r1(h, r):
        k = (second[h] + r) % 4
        wait(recv1.at[h, r], s1r.at[h, r])
        for a in range(4):
            t = block(a, h, first[h], k)
            for j in range(3):
                t += decoded(recv1[h, r, j, a], PAIR_TOP)
            if r:
                send2[h, r - 1, a] = encoded(t, FOUR_TOP)
            else:
                acc[h, a] = t
        if r:
            remote(send2.at[h, r - 1], recv2.at[h, r - 1], sent.at[2], s2r.at[h], ahead(1 - h, r))

    stepped = (sm, sq, sk, sv)

    def r2(h):
        wait(recv2.at[h], s2r.at[h])
        for a in range(4):
            t = acc[h, a]
            for j in range(3):
                t += decoded(recv2[h, j, a], FOUR_TOP)
            new = mast[a, :, lanes_of(h)] - RATE * t
            stepped[a][:, lanes_of(h)] = new
            gat[h, core, first[h], second[h], a] = new.astype(BF16)
        part = gat.at[h, core, first[h], second[h]]
        for j in (2, 1, 3):
            remote(part, part, sent.at[3], g1r.at[h, j - 1], ahead(1 - h, j))

    def back(axis, h, j):
        return ((first, second)[axis][h] + 4 - j) % 4

    def spread(h, r):
        part = gat.at[h, core, first[h], back(1, h, r)]
        for j in (2, 1, 3):
            remote(part, part, sent.at[4], g2r.at[h, j - 1, r], ahead(h, j))

    def hand_over(h, j, r):
        part = gat.at[h, core, back(0, h, j), back(1, h, r)]
        remote(part, part, sent.at[5], fr.at[h, j, r], partner)

    outs = (cm, cq, ck, cv)

    def place(h, k, j, r):
        f, s = back(0, h, j), back(1, h, r)
        zi, xi = (s, f) if h == 0 else (f, s)
        for a in (1, 2, 3):
            outs[a][zi, xi, k, :, lanes_of(h)] = gat[h, k, f, s, a]

    def g1(h, r):
        wait(gat.at[h, core, first[h], back(1, h, r)], g1r.at[h, r - 1])
        spread(h, r)
        hand_over(h, 0, r)
        place(h, core, 0, r)

    def g2(h, j, r):
        wait(gat.at[h, core, back(0, h, j), back(1, h, r)], g2r.at[h, j - 1, r])
        hand_over(h, j, r)
        place(h, core, j, r)

    def last(h, j, r):
        wait(gat.at[h, 1 - core, back(0, h, j), back(1, h, r)], fr.at[h, j, r])
        place(h, 1 - core, j, r)

    def turn_back(h, zi, xi):
        parts = []
        for xj in (xi, xi + 1):
            for k in range(2):
                f, s = (xj, zi) if h == 0 else (zi, xj)
                parts.append(gat[h, k, f, s, 0])
        lane = (zi * 4 + xi) * 64
        cm[lanes_of(h), lane : lane + 128] = jnp.concatenate(parts, axis=0).T

    def n1():
        wait(npair, nr.at[0])
        nx[x] = nbuf[...] + npair[...]
        for j in (2, 1, 3):
            remote(nx.at[x], nx.at[x], ns.at[1], nr.at[1], ahead(0, j))

    def n2():
        wait(nx.at[pl.ds(0, 3)], nr.at[1])
        nz[z] = ((nx[0] + nx[1]) + nx[2]) + nx[3]
        for j in (2, 1, 3):
            remote(nz.at[z], nz.at[z], ns.at[2], nr.at[2], ahead(1, j))

    def n3():
        wait(nz.at[pl.ds(0, 3)], nr.at[2])
        new = ((nz[0] + nz[1]) + nz[2]) + nz[3]
        cn[...] = new[0].astype(BF16)
        cb[...] = new[1].astype(BF16)
        place = jnp.sum(jnp.where(mine[None], new, 0.0), axis=1)
        slot = ((place[:, 0:32] + place[:, 32:64]) + place[:, 64:96]) + place[:, 96:128]
        sn[...] = slot[0:1]
        sb[...] = slot[1:2]

    for r in ORDER:
        for h in range(2):
            e1(h, r)
    n1()
    for r in ORDER:
        for h in range(2):
            r1(h, r)
    n2()
    for copy in masters:
        copy.wait()
    for h in range(2):
        r2(h)
    for h in range(2):
        spread(h, 0)
        hand_over(h, 0, 0)
        place(h, core, 0, 0)
    n3()
    for r in BACK:
        for h in range(2):
            g1(h, r)
    for r in (0, *BACK):
        for j in BACK:
            for h in range(2):
                g2(h, j, r)
    for i, ref in enumerate((pair, send1, send2, send2, send1)):
        wait(ref, sent.at[i])
    wait(nbuf, ns.at[0])
    wait(nx.at[pl.ds(0, 3)], ns.at[1])
    wait(nz.at[pl.ds(0, 3)], ns.at[2])
    for r in (0, *BACK):
        for j in (0, *BACK):
            for h in range(2):
                last(h, j, r)
    for h in range(2):
        for zi in range(4):
            for xi in (0, 2):
                turn_back(h, zi, xi)
    wait(gat.at[0], sent.at[5])


def placed(*refs):
    sems = refs[24]
    copies = [pltpu.make_async_copy(refs[i], refs[12 + i], sems.at[i]) for i in range(12)]
    for copy in copies:
        copy.start()
    for copy in copies:
        copy.wait()


def per_device(pq, pk, pv, pm, pn, pb, mq, mk, mv, mm, mn, mb):
    blocks = (4, 4, 2, 32, 256)
    hbm = pl.BlockSpec(memory_space=pl.ANY)
    vmem = pl.BlockSpec(memory_space=pltpu.VMEM)
    dma = pltpu.SemaphoreType.DMA
    gathered = jax.ShapeDtypeStruct((4, 4, 2, 32, 256), BF16)
    share = jax.ShapeDtypeStruct((32, 256), F32)
    small = jax.ShapeDtypeStruct((8, 128), BF16)
    slot = jax.ShapeDtypeStruct((1, 32), F32)
    shapes = (jax.ShapeDtypeStruct((256, 1024), BF16), gathered, gathered, gathered, small, small)
    shapes += (share,) * 4 + (slot,) * 2
    out = pl.pallas_call(
        kernel,
        out_shape=tuple(pltpu.VMEM(o.shape, o.dtype) for o in shapes),
        in_specs=[hbm] * 12,
        out_specs=(vmem,) * 12,
        scratch_shapes=[
            pltpu.VMEM((4, *blocks), F32),
            pltpu.VMEM((256, 1024), F32),
            pltpu.VMEM((2, 4, 4, 4, 32, 128), F32),
            pltpu.VMEM((2, 4, 3, 4, 32, 128), BF16),
            pltpu.VMEM((2, 4, 3, 4, 32, 128), BF16),
            pltpu.VMEM((2, 3, 4, 32, 128), BF16),
            pltpu.VMEM((2, 3, 4, 32, 128), BF16),
            pltpu.VMEM((2, 4, 32, 128), F32),
            pltpu.VMEM((2, 2, 4, 4, 4, 32, 128), BF16),
            pltpu.VMEM((4, 32, 256), F32),
            pltpu.VMEM((2, 8, 128), F32),
            pltpu.VMEM((2, 8, 128), F32),
            pltpu.VMEM((4, 2, 8, 128), F32),
            pltpu.VMEM((4, 2, 8, 128), F32),
            pltpu.VMEM((2, 1, 32), F32),
            dma((4,)),
            dma((4,)),
            dma((4,)),
            dma((2, 4)),
            dma((2, 4)),
            dma((2,)),
            dma((2, 3)),
            dma((2, 3, 4)),
            dma((2, 4, 4)),
            dma((6,)),
            dma((3,)),
            dma((3,)),
        ],
        compiler_params=pltpu.CompilerParams(collective_id=0, has_side_effects=True, vmem_limit_bytes=60 * 2**20),
        name="step",
    )(
        pm[0], pq.reshape(blocks), pk.reshape(blocks), pv.reshape(blocks), pn.reshape(8, 128), pb.reshape(8, 128),
        mm.T, mq, mk, mv, mn.reshape(1, 32), mb.reshape(1, 32),
    )
    cm, cq, ck, cv, cn, cb, sm, sq, sk, sv, sn, sb = pl.pallas_call(
        placed,
        out_shape=shapes,
        in_specs=[vmem] * 12,
        out_specs=(hbm,) * 12,
        scratch_shapes=[dma((12,))],
        name="placed",
    )(*[pltpu.with_memory_space_constraint(o, pltpu.VMEM) for o in out])
    whole = (1024, 256)
    return (
        cq.reshape(whole), ck.reshape(whole), cv.reshape(whole), cm, cn.reshape(1024), cb.reshape(1024),
        sq, sk, sv, sm.T, sn.reshape(32), sb.reshape(32),
    )


def solution(mesh):
    in_specs = (
        P("batch", None, "cols"),
        P("batch", None, "cols"),
        P("batch", None, "cols"),
        P("batch", "cols", None),
        P("batch", None),
        P("batch", None),
        P("batch", "cols"),
        P("batch", "cols"),
        P("batch", "cols"),
        P("cols", "batch"),
        P("batch"),
        P("batch"),
    )
    out_specs = (
        P(None, "cols"),
        P(None, "cols"),
        P(None, "cols"),
        P("cols", None),
        P(),
        P(),
        P("batch", "cols"),
        P("batch", "cols"),
        P("batch", "cols"),
        P("cols", "batch"),
        P("batch"),
        P("batch"),
    )
    return jax.shard_map(per_device, mesh=mesh, in_specs=in_specs, out_specs=out_specs, check_vma=False)
```

```python
import math

import jax
import jax.numpy as jnp
from jax import lax
from jax.experimental import pallas as pl
from jax.experimental.pallas import tpu as pltpu
from jax.sharding import PartitionSpec as P

MESH = pl.DeviceIdType.MESH
F32 = jnp.float32
BF16 = jnp.bfloat16

RATE = 0.4 * 32**-0.5

SPREAD = 21.0
STEPS = 4096.0
SHIFT = 125.0
PAIR_TOP = 2.6
ORDER = (2, 1, 3, 0)
BACK = (1, 3, 2)
FOUR_TOP = 10.4


def encoded(x, top):
    log = jnp.log(1.0 + jnp.abs(x) * (STEPS / top))
    v = jnp.exp2(log * (SPREAD / math.log(2.0)) - SHIFT)
    return jnp.where(x < 0, -v, v).astype(BF16)


def decoded(code, top):
    v = code.astype(F32)
    log = jnp.log(jnp.abs(v))
    size = (jnp.exp2(log * (1.0 / (SPREAD * math.log(2.0))) + SHIFT / SPREAD) - 1.0) * (top / STEPS)
    return jnp.where(v < 0, -size, size)


def kernel(
    pm, pq, pk, pv, pn, pb, mm, mq, mk, mv, mn, mb,
    cm, cq, ck, cv, cn, cb, sm, sq, sk, sv, sn, sb,
    raw, flat, pair, send1, recv1, send2, recv2, acc, gat, mast,
    nbuf, npair, nx, nz, nmast,
    load_sem, mload_sem, nload_sem, d_recv, s1r, s2r, g1r, g2r, fr, sent, ns, nr, hands,
):
    b = lax.axis_index("batch")
    col = lax.axis_index("cols")
    z, x, core = b // 8, (b // 2) % 4, b % 2
    first, second = (x, z), (z, x)

    def at(z, x, core):
        return (z * 8 + x * 2 + core, col)

    def ahead(axis, j):
        return at(z, (x + j) % 4, core) if axis == 0 else at((z + j) % 4, x, core)

    def wait(ref, sem):
        pltpu.make_async_copy(ref, ref, sem).wait()

    def remote(src, dst, ssem, rsem, dev):
        pltpu.make_async_remote_copy(
            src_ref=src, dst_ref=dst, send_sem=ssem, recv_sem=rsem, device_id=dev, device_id_type=MESH
        ).start()

    def lanes_of(h):
        return slice(128 * h, 128 * h + 128)

    def piece(ref, h, k, core=None):
        cores = slice(None) if core is None else core
        return ref.at[k, :, cores, :, lanes_of(h)] if h == 0 else ref.at[:, k, cores, :, lanes_of(h)]

    def pieces(g, h, k, core):
        ref = raw.at[g]
        return ref.at[:, k, :, core, :, lanes_of(h)] if h == 0 else ref.at[:, :, k, core, :, lanes_of(h)]

    barrier = pltpu.get_barrier_semaphore()
    partner = at(z, x, 1 - core)
    far = [ahead(axis, j) for j in (2, 1, 3) for axis in (0, 1)]

    @pl.when(core == 1)
    def _():
        pl.semaphore_signal(barrier, inc=1, device_id=partner, device_id_type=MESH)

    turned = pltpu.make_async_copy(pm, flat, mload_sem.at[4])
    loads = {
        (h, r, i): pltpu.make_async_copy(
            piece(ref, h, (second[h] + r) % 4), piece(raw.at[0, i], h, (second[h] + r) % 4), load_sem.at[h, r, i]
        )
        for r in ORDER
        for h in range(2)
        for i, ref in enumerate((pq, pk))
    }
    value = pltpu.make_async_copy(pv, raw.at[1, 1], mload_sem.at[5])
    small = [
        pltpu.make_async_copy(pn, nbuf.at[0], nload_sem.at[0]),
        pltpu.make_async_copy(pb, nbuf.at[1], nload_sem.at[1]),
        pltpu.make_async_copy(mn, nmast.at[0], nload_sem.at[2]),
        pltpu.make_async_copy(mb, nmast.at[1], nload_sem.at[3]),
    ]
    masters = [pltpu.make_async_copy(ref, mast.at[a], mload_sem.at[a]) for a, ref in enumerate((mq, mk, mm, mv))]
    for copy in (*loads.values(), *small, turned, value, *masters):
        copy.start()

    def share(g, h, r):
        k = (second[h] + r) % 4
        remote(pieces(g, h, k, 1 - core), pair.at[g, h, k], sent.at[0], d_recv.at[g, h, r], partner)

    @pl.when(core == 0)
    def _():
        pl.semaphore_wait(barrier, 1)
        pl.semaphore_signal(hands, inc=1, device_id=partner, device_id_type=MESH)

    @pl.when(core == 1)
    def _():
        pl.semaphore_wait(hands, 1)
        for peer in far:
            pl.semaphore_signal(barrier, inc=1, device_id=peer, device_id_type=MESH)

    for r in ORDER:
        for h in range(2):
            for i in range(2):
                loads[h, r, i].wait()
            share(0, h, r)

    for copy in small:
        copy.wait()
    lanes = lax.broadcasted_iota(jnp.int32, (8, 128), 1)
    rows = lax.broadcasted_iota(jnp.int32, (8, 128), 0)
    mine = (rows * 4 + lanes // 32) == b
    for i in range(2):
        m = jnp.concatenate([nmast[i]] * 4, axis=1)
        nbuf[i] = jnp.where(mine, jnp.broadcast_to(m, (8, 128)), 0.0) - RATE * nbuf[i]
    remote(nbuf, npair, ns.at[0], nr.at[0], partner)

    def turn(c):
        raw[1, 0, c] = flat[:, 256 * c : 256 * c + 256].T.reshape(4, 2, 32, 256)

    def block(g, i, h, f, k):
        zi, xi = (k, f) if h == 0 else (f, k)
        return raw[g, i, zi, xi, core, :, lanes_of(h)] + pair[g, h, k, i, f]

    def e1(g, h, r):
        k = (second[h] + r) % 4
        wait(pair.at[g, h, k], d_recv.at[g, h, r])
        for j in (2, 1, 3):
            for i in range(2):
                send1[g, h, r, j - 1, i] = encoded(block(g, i, h, (first[h] + j) % 4, k), PAIR_TOP)
            remote(send1.at[g, h, r, j - 1], recv1.at[g, h, r, j - 1], sent.at[1], s1r.at[g, h, r], ahead(h, j))

    def r1(g, h, r):
        k = (second[h] + r) % 4
        wait(recv1.at[g, h, r], s1r.at[g, h, r])
        for i in range(2):
            t = block(g, i, h, first[h], k)
            for j in range(3):
                t += decoded(recv1[g, h, r, j, i], PAIR_TOP)
            if r:
                send2[g, h, r - 1, i] = encoded(t, FOUR_TOP)
            else:
                acc[g, h, i] = t
        if r:
            remote(send2.at[g, h, r - 1], recv2.at[g, h, r - 1], sent.at[2], s2r.at[g, h], ahead(1 - h, r))

    stepped = (sq, sk, sm, sv)

    def r2(g, h):
        wait(recv2.at[g, h], s2r.at[g, h])
        for i in range(2):
            t = acc[g, h, i]
            for j in range(3):
                t += decoded(recv2[g, h, j, i], FOUR_TOP)
            new = mast[2 * g + i, :, lanes_of(h)] - RATE * t
            stepped[2 * g + i][:, lanes_of(h)] = new
            gat[g, h, core, first[h], second[h], i] = new.astype(BF16)
        part = gat.at[g, h, core, first[h], second[h]]
        for j in (2, 1, 3):
            remote(part, part, sent.at[3], g1r.at[g, h, j - 1], ahead(1 - h, j))

    def back(axis, h, j):
        return ((first, second)[axis][h] + 4 - j) % 4

    def spread(g, h, r):
        part = gat.at[g, h, core, first[h], back(1, h, r)]
        for j in (2, 1, 3):
            remote(part, part, sent.at[4], g2r.at[g, h, j - 1, r], ahead(h, j))

    def hand_over(g, h, j, r):
        part = gat.at[g, h, core, back(0, h, j), back(1, h, r)]
        remote(part, part, sent.at[5], fr.at[g, h, j, r], partner)

    outs = (cq, ck, cm, cv)

    def place(g, h, k, j, r):
        f, s = back(0, h, j), back(1, h, r)
        zi, xi = (s, f) if h == 0 else (f, s)
        for i in range(2):
            if 2 * g + i != 2:
                outs[2 * g + i][zi, xi, k, :, lanes_of(h)] = gat[g, h, k, f, s, i]

    def own(g, h):
        spread(g, h, 0)
        hand_over(g, h, 0, 0)
        place(g, h, core, 0, 0)

    def g1(g, h, r):
        wait(gat.at[g, h, core, first[h], back(1, h, r)], g1r.at[g, h, r - 1])
        spread(g, h, r)
        hand_over(g, h, 0, r)
        place(g, h, core, 0, r)

    def g2(g, h, j, r):
        wait(gat.at[g, h, core, back(0, h, j), back(1, h, r)], g2r.at[g, h, j - 1, r])
        hand_over(g, h, j, r)
        place(g, h, core, j, r)

    def last(g, h, j, r):
        wait(gat.at[g, h, 1 - core, back(0, h, j), back(1, h, r)], fr.at[g, h, j, r])
        place(g, h, 1 - core, j, r)

    def turn_back(h, zi, xi):
        parts = []
        for xj in (xi, xi + 1):
            for k in range(2):
                f, s = (xj, zi) if h == 0 else (zi, xj)
                parts.append(gat[1, h, k, f, s, 0])
        lane = pl.multiple_of((zi * 4 + xi) * 64, 128)
        cm[lanes_of(h), pl.ds(lane, 128)] = jnp.concatenate(parts, axis=0).T

    def finish(g, r):
        for j in (0, *BACK):
            for h in range(2):
                last(g, h, j, r)
        if g == 1:
            for xi in (0, 2):
                turn_back(0, back(1, 0, r), xi)

    def n1():
        wait(npair, nr.at[0])
        nx[x] = nbuf[...] + npair[...]
        for j in (2, 1, 3):
            remote(nx.at[x], nx.at[x], ns.at[1], nr.at[1], ahead(0, j))

    def n2():
        wait(nx.at[pl.ds(0, 3)], nr.at[1])
        nz[z] = ((nx[0] + nx[1]) + nx[2]) + nx[3]
        for j in (2, 1, 3):
            remote(nz.at[z], nz.at[z], ns.at[2], nr.at[2], ahead(1, j))

    def n3():
        wait(nz.at[pl.ds(0, 3)], nr.at[2])
        new = ((nz[0] + nz[1]) + nz[2]) + nz[3]
        cn[...] = new[0].astype(BF16)
        cb[...] = new[1].astype(BF16)
        place = jnp.sum(jnp.where(mine[None], new, 0.0), axis=1)
        slot = ((place[:, 0:32] + place[:, 32:64]) + place[:, 64:96]) + place[:, 96:128]
        sn[...] = slot[0:1]
        sb[...] = slot[1:2]

    both = range(2)

    def over(stage, g, *choices):
        for c in choices:
            for h in both:
                stage(g, h, *(c if isinstance(c, tuple) else (c,)))

    def gathered(g):
        before = None
        for r in (0, *BACK):
            over(g2, g, *((j, r) for j in BACK))
            if before is not None:
                finish(g, before)
            before = r

    @pl.when(core == 1)
    def _():
        pl.semaphore_wait(barrier, 6)
        pl.semaphore_signal(hands, inc=1, device_id=partner, device_id_type=MESH)

    @pl.when(core == 0)
    def _():
        pl.semaphore_wait(hands, 1)

    over(e1, 0, 2)
    turned.wait()
    turn(0)
    turn(1)
    over(e1, 0, 1)
    turn(2)
    turn(3)
    value.wait()
    over(share, 1, *ORDER)
    over(e1, 0, 3, 0)
    over(e1, 1, *ORDER)
    n1()
    over(r1, 0, *ORDER)
    for copy in masters:
        copy.wait()
    over(r1, 1, *ORDER)
    over(r2, 0, ())
    over(own, 0, ())
    n2()
    over(r2, 1, ())
    over(own, 1, ())
    over(g1, 0, 1, 3, 2)
    over(g1, 1, 1, 3, 2)
    n3()
    gathered(0)
    over(g2, 1, *((j, 0) for j in BACK))
    over(g2, 1, *((j, 1) for j in BACK))
    finish(1, 0)
    finish(0, 2)
    over(g2, 1, *((j, 3) for j in BACK))
    finish(1, 1)
    over(g2, 1, *((j, 2) for j in BACK))
    finish(1, 3)
    for zi in range(4):
        turn_back(1, zi, x // 2 * 2)
    for i, ref in enumerate((pair, send1, send2, send2, send1)):
        wait(ref, sent.at[i])
    wait(nbuf, ns.at[0])
    wait(nx.at[pl.ds(0, 3)], ns.at[1])
    wait(nz.at[pl.ds(0, 3)], ns.at[2])
    finish(1, 2)
    for zi in range(4):
        turn_back(1, zi, 2 - x // 2 * 2)
    wait(gat.at[:, 0], sent.at[5])


def placed(*refs):
    sems = refs[24]
    copies = [pltpu.make_async_copy(refs[i], refs[12 + i], sems.at[i]) for i in range(12)]
    for copy in copies:
        copy.start()
    for copy in copies:
        copy.wait()


def per_device(pq, pk, pv, pm, pn, pb, mq, mk, mv, mm, mn, mb):
    blocks = (4, 4, 2, 32, 256)
    hbm = pl.BlockSpec(memory_space=pl.ANY)
    vmem = pl.BlockSpec(memory_space=pltpu.VMEM)
    dma = pltpu.SemaphoreType.DMA
    gathered = jax.ShapeDtypeStruct((4, 4, 2, 32, 256), BF16)
    share = jax.ShapeDtypeStruct((32, 256), F32)
    small = jax.ShapeDtypeStruct((8, 128), BF16)
    slot = jax.ShapeDtypeStruct((1, 32), F32)
    shapes = (jax.ShapeDtypeStruct((256, 1024), BF16), gathered, gathered, gathered, small, small)
    shapes += (share,) * 4 + (slot,) * 2
    out = pl.pallas_call(
        kernel,
        out_shape=tuple(pltpu.VMEM(o.shape, o.dtype) for o in shapes),
        in_specs=[hbm] * 12,
        out_specs=(vmem,) * 12,
        scratch_shapes=[
            pltpu.VMEM((2, 2, *blocks), F32),
            pltpu.VMEM((256, 1024), F32),
            pltpu.VMEM((2, 2, 4, 2, 4, 32, 128), F32),
            pltpu.VMEM((2, 2, 4, 3, 2, 32, 128), BF16),
            pltpu.VMEM((2, 2, 4, 3, 2, 32, 128), BF16),
            pltpu.VMEM((2, 2, 3, 2, 32, 128), BF16),
            pltpu.VMEM((2, 2, 3, 2, 32, 128), BF16),
            pltpu.VMEM((2, 2, 2, 32, 128), F32),
            pltpu.VMEM((2, 2, 2, 4, 4, 2, 32, 128), BF16),
            pltpu.VMEM((4, 32, 256), F32),
            pltpu.VMEM((2, 8, 128), F32),
            pltpu.VMEM((2, 8, 128), F32),
            pltpu.VMEM((4, 2, 8, 128), F32),
            pltpu.VMEM((4, 2, 8, 128), F32),
            pltpu.VMEM((2, 1, 32), F32),
            dma((2, 4, 2)),
            dma((6,)),
            dma((4,)),
            dma((2, 2, 4)),
            dma((2, 2, 4)),
            dma((2, 2)),
            dma((2, 2, 3)),
            dma((2, 2, 3, 4)),
            dma((2, 2, 4, 4)),
            dma((6,)),
            dma((3,)),
            dma((3,)),
            pltpu.SemaphoreType.REGULAR,
        ],
        compiler_params=pltpu.CompilerParams(collective_id=0, has_side_effects=True, vmem_limit_bytes=60 * 2**20),
        name="step",
    )(
        pm[0], pq.reshape(blocks), pk.reshape(blocks), pv.reshape(blocks), pn.reshape(8, 128), pb.reshape(8, 128),
        mm.T, mq, mk, mv, mn.reshape(1, 32), mb.reshape(1, 32),
    )
    cm, cq, ck, cv, cn, cb, sm, sq, sk, sv, sn, sb = pl.pallas_call(
        placed,
        out_shape=shapes,
        in_specs=[vmem] * 12,
        out_specs=(hbm,) * 12,
        scratch_shapes=[dma((12,))],
        name="placed",
    )(*[pltpu.with_memory_space_constraint(o, pltpu.VMEM) for o in out])
    whole = (1024, 256)
    return (
        cq.reshape(whole), ck.reshape(whole), cv.reshape(whole), cm, cn.reshape(1024), cb.reshape(1024),
        sq, sk, sv, sm.T, sn.reshape(32), sb.reshape(32),
    )


def solution(mesh):
    in_specs = (
        P("batch", None, "cols"),
        P("batch", None, "cols"),
        P("batch", None, "cols"),
        P("batch", "cols", None),
        P("batch", None),
        P("batch", None),
        P("batch", "cols"),
        P("batch", "cols"),
        P("batch", "cols"),
        P("cols", "batch"),
        P("batch"),
        P("batch"),
    )
    out_specs = (
        P(None, "cols"),
        P(None, "cols"),
        P(None, "cols"),
        P("cols", None),
        P(),
        P(),
        P("batch", "cols"),
        P("batch", "cols"),
        P("batch", "cols"),
        P("cols", "batch"),
        P("batch"),
        P("batch"),
    )
    return jax.shard_map(per_device, mesh=mesh, in_specs=in_specs, out_specs=out_specs, check_vma=False)
```

```python
import math

import jax
import jax.numpy as jnp
from jax import lax
from jax.experimental import pallas as pl
from jax.experimental.pallas import tpu as pltpu
from jax.sharding import PartitionSpec as P

MESH = pl.DeviceIdType.MESH
F32 = jnp.float32
BF16 = jnp.bfloat16

RATE = 0.4 * 32**-0.5

SPREAD = 21.0
STEPS = 4096.0
SHIFT = 125.0
PAIR_TOP = 2.6
ORDER = (2, 1, 3, 0)
LATE = ((1, 2), (1, 3))
BACK = (1, 3, 2)
FOUR_TOP = 10.4


def encoded(x, top):
    log = jnp.log(1.0 + jnp.abs(x) * (STEPS / top))
    v = jnp.exp2(log * (SPREAD / math.log(2.0)) - SHIFT)
    return jnp.where(x < 0, -v, v).astype(BF16)


def decoded(code, top):
    v = code.astype(F32)
    log = jnp.log(jnp.abs(v))
    size = (jnp.exp2(log * (1.0 / (SPREAD * math.log(2.0))) + SHIFT / SPREAD) - 1.0) * (top / STEPS)
    return jnp.where(v < 0, -size, size)


def kernel(
    pm, pq, pk, pv, pn, pb, mm, mq, mk, mv, mn, mb,
    cm, cq, ck, cv, cn, cb, sm, sq, sk, sv, sn, sb,
    raw, flat, pair, send1, recv1, send2, recv2, acc, gat, mast,
    nbuf, npair, nx, nz, nmast,
    load_sem, mload_sem, nload_sem, d_recv, s1r, s2r, g1r, g2r, fr, sent, ns, nr, hands,
):
    b = lax.axis_index("batch")
    col = lax.axis_index("cols")
    z, x, core = b // 8, (b // 2) % 4, b % 2
    first, second = (x, z), (z, x)

    def at(z, x, core):
        return (z * 8 + x * 2 + core, col)

    def ahead(axis, j, core=core):
        return at(z, (x + j) % 4, core) if axis == 0 else at((z + j) % 4, x, core)

    def wait(ref, sem):
        pltpu.make_async_copy(ref, ref, sem).wait()

    def remote(src, dst, ssem, rsem, dev):
        pltpu.make_async_remote_copy(
            src_ref=src, dst_ref=dst, send_sem=ssem, recv_sem=rsem, device_id=dev, device_id_type=MESH
        ).start()

    def lanes_of(h):
        return slice(128 * h, 128 * h + 128)

    def piece(ref, h, k, core=None):
        cores = slice(None) if core is None else core
        return ref.at[k, :, cores, :, lanes_of(h)] if h == 0 else ref.at[:, k, cores, :, lanes_of(h)]

    def pieces(g, h, k, core):
        ref = raw.at[g]
        return ref.at[:, k, :, core, :, lanes_of(h)] if h == 0 else ref.at[:, :, k, core, :, lanes_of(h)]

    barrier = pltpu.get_barrier_semaphore()
    partner = at(z, x, 1 - core)
    far = [ahead(axis, j) for j in (2, 1, 3) for axis in (0, 1)]

    @pl.when(core == 1)
    def _():
        pl.semaphore_signal(barrier, inc=1, device_id=partner, device_id_type=MESH)

    turned = pltpu.make_async_copy(pm, flat, mload_sem.at[4])
    loads = {
        (h, r, i): pltpu.make_async_copy(
            piece(ref, h, (second[h] + r) % 4), piece(raw.at[0, i], h, (second[h] + r) % 4), load_sem.at[h, r, i]
        )
        for r in ORDER
        for h in range(2)
        for i, ref in enumerate((pq, pk))
    }
    value = pltpu.make_async_copy(pv, raw.at[1, 1], mload_sem.at[5])
    small = [
        pltpu.make_async_copy(pn, nbuf.at[0], nload_sem.at[0]),
        pltpu.make_async_copy(pb, nbuf.at[1], nload_sem.at[1]),
        pltpu.make_async_copy(mn, nmast.at[0], nload_sem.at[2]),
        pltpu.make_async_copy(mb, nmast.at[1], nload_sem.at[3]),
    ]
    masters = [pltpu.make_async_copy(ref, mast.at[a], mload_sem.at[a]) for a, ref in enumerate((mq, mk, mm, mv))]
    for copy in (*loads.values(), *small, turned, value, *masters):
        copy.start()

    def share(g, h, r):
        k = (second[h] + r) % 4
        remote(pieces(g, h, k, 1 - core), pair.at[g, h, k], sent.at[0], d_recv.at[g, h, r], partner)

    @pl.when(core == 0)
    def _():
        pl.semaphore_wait(barrier, 1)
        pl.semaphore_signal(hands, inc=1, device_id=partner, device_id_type=MESH)

    @pl.when(core == 1)
    def _():
        pl.semaphore_wait(hands, 1)
        for peer in far:
            pl.semaphore_signal(barrier, inc=1, device_id=peer, device_id_type=MESH)

    for r in ORDER:
        for h in range(2):
            for i in range(2):
                loads[h, r, i].wait()
            share(0, h, r)

    for copy in small:
        copy.wait()
    lanes = lax.broadcasted_iota(jnp.int32, (8, 128), 1)
    rows = lax.broadcasted_iota(jnp.int32, (8, 128), 0)
    mine = (rows * 4 + lanes // 32) == b
    for i in range(2):
        m = jnp.concatenate([nmast[i]] * 4, axis=1)
        nbuf[i] = jnp.where(mine, jnp.broadcast_to(m, (8, 128)), 0.0) - RATE * nbuf[i]
    remote(nbuf, npair, ns.at[0], nr.at[0], partner)

    def turn(c):
        raw[1, 0, c] = flat[:, 256 * c : 256 * c + 256].T.reshape(4, 2, 32, 256)

    def block(g, i, h, f, k):
        zi, xi = (k, f) if h == 0 else (f, k)
        return raw[g, i, zi, xi, core, :, lanes_of(h)] + pair[g, h, k, i, f]

    def e1(g, h, r):
        k = (second[h] + r) % 4
        wait(pair.at[g, h, k], d_recv.at[g, h, r])
        for j in (2, 1, 3):
            for i in range(2):
                send1[g, h, r, j - 1, i] = encoded(block(g, i, h, (first[h] + j) % 4, k), PAIR_TOP)
            remote(send1.at[g, h, r, j - 1], recv1.at[g, h, r, j - 1], sent.at[1], s1r.at[g, h, r], ahead(h, j))

    def r1(g, h, r):
        k = (second[h] + r) % 4
        wait(recv1.at[g, h, r], s1r.at[g, h, r])
        for i in range(2):
            t = block(g, i, h, first[h], k)
            for j in range(3):
                t += decoded(recv1[g, h, r, j, i], PAIR_TOP)
            if r:
                send2[g, h, r - 1, i] = encoded(t, FOUR_TOP)
            else:
                acc[g, h, i] = t
        if r:
            remote(send2.at[g, h, r - 1], recv2.at[g, h, r - 1], sent.at[2], s2r.at[g, h], ahead(1 - h, r))

    stepped = (sq, sk, sm, sv)

    def r2(g, h):
        wait(recv2.at[g, h], s2r.at[g, h])
        for i in range(2):
            t = acc[g, h, i]
            for j in range(3):
                t += decoded(recv2[g, h, j, i], FOUR_TOP)
            new = mast[2 * g + i, :, lanes_of(h)] - RATE * t
            stepped[2 * g + i][:, lanes_of(h)] = new
            gat[g, h, core, first[h], second[h], i] = new.astype(BF16)
        part = gat.at[g, h, core, first[h], second[h]]
        for j in (2, 1, 3):
            remote(part, part, sent.at[3], g1r.at[g, h, j - 1], ahead(1 - h, j))

    def back(axis, h, j):
        return ((first, second)[axis][h] + 4 - j) % 4

    def spread(g, h, r):
        part = gat.at[g, h, core, first[h], back(1, h, r)]
        for j in (2, 1, 3):
            remote(part, part, sent.at[4], g2r.at[g, h, j - 1, r], ahead(h, j))
        for j in (2, 1, 3) if (g, r) in LATE else ():
            remote(part, part, sent.at[5], fr.at[g, h, j, r], ahead(h, j, 1 - core))

    def hand_over(g, h, j, r):
        part = gat.at[g, h, core, back(0, h, j), back(1, h, r)]
        remote(part, part, sent.at[5], fr.at[g, h, j, r], partner)

    outs = (cq, ck, cm, cv)

    def place(g, h, k, j, r):
        f, s = back(0, h, j), back(1, h, r)
        zi, xi = (s, f) if h == 0 else (f, s)
        for i in range(2):
            if 2 * g + i != 2:
                outs[2 * g + i][zi, xi, k, :, lanes_of(h)] = gat[g, h, k, f, s, i]

    def own(g, h):
        spread(g, h, 0)
        hand_over(g, h, 0, 0)
        place(g, h, core, 0, 0)

    def g1(g, h, r):
        wait(gat.at[g, h, core, first[h], back(1, h, r)], g1r.at[g, h, r - 1])
        spread(g, h, r)
        hand_over(g, h, 0, r)
        place(g, h, core, 0, r)

    def g2(g, h, j, r):
        wait(gat.at[g, h, core, back(0, h, j), back(1, h, r)], g2r.at[g, h, j - 1, r])
        if (g, r) not in LATE:
            hand_over(g, h, j, r)
        place(g, h, core, j, r)

    def last(g, h, j, r):
        wait(gat.at[g, h, 1 - core, back(0, h, j), back(1, h, r)], fr.at[g, h, j, r])
        place(g, h, 1 - core, j, r)

    def turn_back(h, zi, xi):
        parts = []
        for xj in (xi, xi + 1):
            for k in range(2):
                f, s = (xj, zi) if h == 0 else (zi, xj)
                parts.append(gat[1, h, k, f, s, 0])
        lane = pl.multiple_of((zi * 4 + xi) * 64, 128)
        cm[lanes_of(h), pl.ds(lane, 128)] = jnp.concatenate(parts, axis=0).T

    def finish(g, r):
        for j in (0, *BACK):
            for h in range(2):
                last(g, h, j, r)
        if g == 1:
            for xi in (0, 2):
                turn_back(0, back(1, 0, r), xi)

    def n1():
        wait(npair, nr.at[0])
        nx[x] = nbuf[...] + npair[...]
        for j in (2, 1, 3):
            remote(nx.at[x], nx.at[x], ns.at[1], nr.at[1], ahead(0, j))

    def n2():
        wait(nx.at[pl.ds(0, 3)], nr.at[1])
        nz[z] = ((nx[0] + nx[1]) + nx[2]) + nx[3]
        for j in (2, 1, 3):
            remote(nz.at[z], nz.at[z], ns.at[2], nr.at[2], ahead(1, j))

    def n3():
        wait(nz.at[pl.ds(0, 3)], nr.at[2])
        new = ((nz[0] + nz[1]) + nz[2]) + nz[3]
        cn[...] = new[0].astype(BF16)
        cb[...] = new[1].astype(BF16)
        place = jnp.sum(jnp.where(mine[None], new, 0.0), axis=1)
        slot = ((place[:, 0:32] + place[:, 32:64]) + place[:, 64:96]) + place[:, 96:128]
        sn[...] = slot[0:1]
        sb[...] = slot[1:2]

    both = range(2)

    def over(stage, g, *choices):
        for c in choices:
            for h in both:
                stage(g, h, *(c if isinstance(c, tuple) else (c,)))

    def gathered(g):
        before = None
        for r in (0, *BACK):
            over(g2, g, *((j, r) for j in BACK))
            if before is not None:
                finish(g, before)
            before = r

    @pl.when(core == 1)
    def _():
        pl.semaphore_wait(barrier, 6)
        pl.semaphore_signal(hands, inc=1, device_id=partner, device_id_type=MESH)

    @pl.when(core == 0)
    def _():
        pl.semaphore_wait(hands, 1)

    over(e1, 0, 2)
    turned.wait()
    turn(0)
    turn(1)
    over(e1, 0, 1)
    turn(2)
    turn(3)
    value.wait()
    over(share, 1, *ORDER)
    over(e1, 0, 3, 0)
    over(e1, 1, *ORDER)
    n1()
    over(r1, 0, *ORDER)
    for copy in masters:
        copy.wait()
    over(r1, 1, *ORDER)
    over(r2, 0, ())
    over(own, 0, ())
    n2()
    over(r2, 1, ())
    over(own, 1, ())
    over(g1, 0, 1, 3, 2)
    over(g1, 1, 1, 3, 2)
    n3()
    gathered(0)
    over(g2, 1, *((j, 0) for j in BACK))
    over(g2, 1, *((j, 1) for j in BACK))
    finish(1, 0)
    finish(0, 2)
    over(g2, 1, *((j, 3) for j in BACK))
    finish(1, 1)
    over(g2, 1, *((j, 2) for j in BACK))
    finish(1, 3)
    for zi in range(4):
        turn_back(1, zi, x // 2 * 2)
    for i, ref in enumerate((pair, send1, send2, send2, send1)):
        wait(ref, sent.at[i])
    wait(nbuf, ns.at[0])
    wait(nx.at[pl.ds(0, 3)], ns.at[1])
    wait(nz.at[pl.ds(0, 3)], ns.at[2])
    finish(1, 2)
    for zi in range(4):
        turn_back(1, zi, 2 - x // 2 * 2)
    wait(gat.at[:, 0], sent.at[5])


def placed(*refs):
    sems = refs[24]
    copies = [pltpu.make_async_copy(refs[i], refs[12 + i], sems.at[i]) for i in range(12)]
    for copy in copies:
        copy.start()
    for copy in copies:
        copy.wait()


def per_device(pq, pk, pv, pm, pn, pb, mq, mk, mv, mm, mn, mb):
    blocks = (4, 4, 2, 32, 256)
    hbm = pl.BlockSpec(memory_space=pl.ANY)
    vmem = pl.BlockSpec(memory_space=pltpu.VMEM)
    dma = pltpu.SemaphoreType.DMA
    gathered = jax.ShapeDtypeStruct((4, 4, 2, 32, 256), BF16)
    share = jax.ShapeDtypeStruct((32, 256), F32)
    small = jax.ShapeDtypeStruct((8, 128), BF16)
    slot = jax.ShapeDtypeStruct((1, 32), F32)
    shapes = (jax.ShapeDtypeStruct((256, 1024), BF16), gathered, gathered, gathered, small, small)
    shapes += (share,) * 4 + (slot,) * 2
    out = pl.pallas_call(
        kernel,
        out_shape=tuple(pltpu.VMEM(o.shape, o.dtype) for o in shapes),
        in_specs=[hbm] * 12,
        out_specs=(vmem,) * 12,
        scratch_shapes=[
            pltpu.VMEM((2, 2, *blocks), F32),
            pltpu.VMEM((256, 1024), F32),
            pltpu.VMEM((2, 2, 4, 2, 4, 32, 128), F32),
            pltpu.VMEM((2, 2, 4, 3, 2, 32, 128), BF16),
            pltpu.VMEM((2, 2, 4, 3, 2, 32, 128), BF16),
            pltpu.VMEM((2, 2, 3, 2, 32, 128), BF16),
            pltpu.VMEM((2, 2, 3, 2, 32, 128), BF16),
            pltpu.VMEM((2, 2, 2, 32, 128), F32),
            pltpu.VMEM((2, 2, 2, 4, 4, 2, 32, 128), BF16),
            pltpu.VMEM((4, 32, 256), F32),
            pltpu.VMEM((2, 8, 128), F32),
            pltpu.VMEM((2, 8, 128), F32),
            pltpu.VMEM((4, 2, 8, 128), F32),
            pltpu.VMEM((4, 2, 8, 128), F32),
            pltpu.VMEM((2, 1, 32), F32),
            dma((2, 4, 2)),
            dma((6,)),
            dma((4,)),
            dma((2, 2, 4)),
            dma((2, 2, 4)),
            dma((2, 2)),
            dma((2, 2, 3)),
            dma((2, 2, 3, 4)),
            dma((2, 2, 4, 4)),
            dma((6,)),
            dma((3,)),
            dma((3,)),
            pltpu.SemaphoreType.REGULAR,
        ],
        compiler_params=pltpu.CompilerParams(collective_id=0, has_side_effects=True, vmem_limit_bytes=60 * 2**20),
        name="step",
    )(
        pm[0], pq.reshape(blocks), pk.reshape(blocks), pv.reshape(blocks), pn.reshape(8, 128), pb.reshape(8, 128),
        mm.T, mq, mk, mv, mn.reshape(1, 32), mb.reshape(1, 32),
    )
    cm, cq, ck, cv, cn, cb, sm, sq, sk, sv, sn, sb = pl.pallas_call(
        placed,
        out_shape=shapes,
        in_specs=[vmem] * 12,
        out_specs=(hbm,) * 12,
        scratch_shapes=[dma((12,))],
        name="placed",
    )(*[pltpu.with_memory_space_constraint(o, pltpu.VMEM) for o in out])
    whole = (1024, 256)
    return (
        cq.reshape(whole), ck.reshape(whole), cv.reshape(whole), cm, cn.reshape(1024), cb.reshape(1024),
        sq, sk, sv, sm.T, sn.reshape(32), sb.reshape(32),
    )


def solution(mesh):
    in_specs = (
        P("batch", None, "cols"),
        P("batch", None, "cols"),
        P("batch", None, "cols"),
        P("batch", "cols", None),
        P("batch", None),
        P("batch", None),
        P("batch", "cols"),
        P("batch", "cols"),
        P("batch", "cols"),
        P("cols", "batch"),
        P("batch"),
        P("batch"),
    )
    out_specs = (
        P(None, "cols"),
        P(None, "cols"),
        P(None, "cols"),
        P("cols", None),
        P(),
        P(),
        P("batch", "cols"),
        P("batch", "cols"),
        P("batch", "cols"),
        P("cols", "batch"),
        P("batch"),
        P("batch"),
    )
    return jax.shard_map(per_device, mesh=mesh, in_specs=in_specs, out_specs=out_specs, check_vma=False)
```

```python
import math

import jax
import jax.numpy as jnp
from jax import lax
from jax.experimental import pallas as pl
from jax.experimental.pallas import tpu as pltpu
from jax.sharding import PartitionSpec as P

MESH = pl.DeviceIdType.MESH
F32 = jnp.float32
BF16 = jnp.bfloat16

RATE = 0.4 * 32**-0.5

SPREAD = 15.75
STEPS = 65536.0
SHIFT = 125.0
PAIR_TOP = 2.6
ORDER = (2, 1, 3, 0)
LATE = ((1, 2), (1, 3))
BACK = (1, 3, 2)
FOUR_TOP = 10.4


def encoded(x, top):
    log = jnp.log(1.0 + jnp.abs(x) * (STEPS / top))
    v = jnp.exp2(log * (SPREAD / math.log(2.0)) - SHIFT)
    return jnp.where(x < 0, -v, v).astype(BF16)


def decoded(code, top):
    v = code.astype(F32)
    log = jnp.log(jnp.abs(v))
    size = (jnp.exp2(log * (1.0 / (SPREAD * math.log(2.0))) + SHIFT / SPREAD) - 1.0) * (top / STEPS)
    return jnp.where(v < 0, -size, size)


def kernel(
    pm, pq, pk, pv, pn, pb, mm, mq, mk, mv, mn, mb,
    cm, cq, ck, cv, cn, cb, sm, sq, sk, sv, sn, sb,
    raw, flat, pair, send1, recv1, send2, recv2, acc, gat, mast,
    nbuf, npair, nx, nz, nmast,
    load_sem, mload_sem, nload_sem, d_recv, s1r, s2r, g1r, g2r, fr, sent, ns, nr, hands,
):
    b = lax.axis_index("batch")
    col = lax.axis_index("cols")
    z, x, core = b // 8, (b // 2) % 4, b % 2
    first, second = (x, z), (z, x)

    def at(z, x, core):
        return (z * 8 + x * 2 + core, col)

    def ahead(axis, j, core=core):
        return at(z, (x + j) % 4, core) if axis == 0 else at((z + j) % 4, x, core)

    def wait(ref, sem):
        pltpu.make_async_copy(ref, ref, sem).wait()

    def remote(src, dst, ssem, rsem, dev):
        pltpu.make_async_remote_copy(
            src_ref=src, dst_ref=dst, send_sem=ssem, recv_sem=rsem, device_id=dev, device_id_type=MESH
        ).start()

    def lanes_of(h):
        return slice(128 * h, 128 * h + 128)

    def piece(ref, h, k, core=None):
        cores = slice(None) if core is None else core
        return ref.at[k, :, cores, :, lanes_of(h)] if h == 0 else ref.at[:, k, cores, :, lanes_of(h)]

    def pieces(g, h, k, core):
        ref = raw.at[g]
        return ref.at[:, k, :, core, :, lanes_of(h)] if h == 0 else ref.at[:, :, k, core, :, lanes_of(h)]

    barrier = pltpu.get_barrier_semaphore()
    partner = at(z, x, 1 - core)
    far = [ahead(axis, j) for j in (2, 1, 3) for axis in (0, 1)]

    @pl.when(core == 1)
    def _():
        pl.semaphore_signal(barrier, inc=1, device_id=partner, device_id_type=MESH)

    turned = pltpu.make_async_copy(pm, flat, mload_sem.at[4])
    loads = {
        (h, r, i): pltpu.make_async_copy(
            piece(ref, h, (second[h] + r) % 4), piece(raw.at[0, i], h, (second[h] + r) % 4), load_sem.at[h, r, i]
        )
        for r in ORDER
        for h in range(2)
        for i, ref in enumerate((pq, pk))
    }
    value = pltpu.make_async_copy(pv, raw.at[1, 1], mload_sem.at[5])
    small = [
        pltpu.make_async_copy(pn, nbuf.at[0], nload_sem.at[0]),
        pltpu.make_async_copy(pb, nbuf.at[1], nload_sem.at[1]),
        pltpu.make_async_copy(mn, nmast.at[0], nload_sem.at[2]),
        pltpu.make_async_copy(mb, nmast.at[1], nload_sem.at[3]),
    ]
    masters = [pltpu.make_async_copy(ref, mast.at[a], mload_sem.at[a]) for a, ref in enumerate((mq, mk, mm, mv))]
    for copy in (*loads.values(), *small, turned, value, *masters):
        copy.start()

    def share(g, h, r):
        k = (second[h] + r) % 4
        remote(pieces(g, h, k, 1 - core), pair.at[g, h, k], sent.at[0], d_recv.at[g, h, r], partner)

    @pl.when(core == 0)
    def _():
        pl.semaphore_wait(barrier, 1)
        pl.semaphore_signal(hands, inc=1, device_id=partner, device_id_type=MESH)

    @pl.when(core == 1)
    def _():
        pl.semaphore_wait(hands, 1)
        for peer in far:
            pl.semaphore_signal(barrier, inc=1, device_id=peer, device_id_type=MESH)

    for r in ORDER:
        for h in range(2):
            for i in range(2):
                loads[h, r, i].wait()
            share(0, h, r)

    for copy in small:
        copy.wait()
    lanes = lax.broadcasted_iota(jnp.int32, (8, 128), 1)
    rows = lax.broadcasted_iota(jnp.int32, (8, 128), 0)
    mine = (rows * 4 + lanes // 32) == b
    for i in range(2):
        m = jnp.concatenate([nmast[i]] * 4, axis=1)
        nbuf[i] = jnp.where(mine, jnp.broadcast_to(m, (8, 128)), 0.0) - RATE * nbuf[i]
    remote(nbuf, npair, ns.at[0], nr.at[0], partner)

    def turn(c):
        raw[1, 0, c] = flat[:, 256 * c : 256 * c + 256].T.reshape(4, 2, 32, 256)

    def block(g, i, h, f, k):
        zi, xi = (k, f) if h == 0 else (f, k)
        return raw[g, i, zi, xi, core, :, lanes_of(h)] + pair[g, h, k, i, f]

    def e1(g, h, r):
        k = (second[h] + r) % 4
        wait(pair.at[g, h, k], d_recv.at[g, h, r])
        for j in (2, 1, 3):
            for i in range(2):
                send1[g, h, r, j - 1, i] = encoded(block(g, i, h, (first[h] + j) % 4, k), PAIR_TOP)
            remote(send1.at[g, h, r, j - 1], recv1.at[g, h, r, j - 1], sent.at[1], s1r.at[g, h, r], ahead(h, j))

    def r1(g, h, r):
        k = (second[h] + r) % 4
        wait(recv1.at[g, h, r], s1r.at[g, h, r])
        for i in range(2):
            t = block(g, i, h, first[h], k)
            for j in range(3):
                t += decoded(recv1[g, h, r, j, i], PAIR_TOP)
            if r:
                send2[g, h, r - 1, i] = encoded(t, FOUR_TOP)
            else:
                acc[g, h, i] = t
        if r:
            remote(send2.at[g, h, r - 1], recv2.at[g, h, r - 1], sent.at[2], s2r.at[g, h], ahead(1 - h, r))

    stepped = (sq, sk, sm, sv)

    def r2(g, h):
        wait(recv2.at[g, h], s2r.at[g, h])
        for i in range(2):
            t = acc[g, h, i]
            for j in range(3):
                t += decoded(recv2[g, h, j, i], FOUR_TOP)
            new = mast[2 * g + i, :, lanes_of(h)] - RATE * t
            stepped[2 * g + i][:, lanes_of(h)] = new
            gat[g, h, core, first[h], second[h], i] = new.astype(BF16)
        part = gat.at[g, h, core, first[h], second[h]]
        for j in (2, 1, 3):
            remote(part, part, sent.at[3], g1r.at[g, h, j - 1], ahead(1 - h, j))

    def back(axis, h, j):
        return ((first, second)[axis][h] + 4 - j) % 4

    def spread(g, h, r):
        part = gat.at[g, h, core, first[h], back(1, h, r)]
        for j in (2, 1, 3):
            remote(part, part, sent.at[4], g2r.at[g, h, j - 1, r], ahead(h, j))
        for j in (2, 1, 3) if (g, r) in LATE else ():
            remote(part, part, sent.at[5], fr.at[g, h, j, r], ahead(h, j, 1 - core))

    def hand_over(g, h, j, r):
        part = gat.at[g, h, core, back(0, h, j), back(1, h, r)]
        remote(part, part, sent.at[5], fr.at[g, h, j, r], partner)

    outs = (cq, ck, cm, cv)

    def place(g, h, k, j, r):
        f, s = back(0, h, j), back(1, h, r)
        zi, xi = (s, f) if h == 0 else (f, s)
        for i in range(2):
            if 2 * g + i != 2:
                outs[2 * g + i][zi, xi, k, :, lanes_of(h)] = gat[g, h, k, f, s, i]

    def own(g, h):
        spread(g, h, 0)
        hand_over(g, h, 0, 0)
        place(g, h, core, 0, 0)

    def g1(g, h, r):
        wait(gat.at[g, h, core, first[h], back(1, h, r)], g1r.at[g, h, r - 1])
        spread(g, h, r)
        hand_over(g, h, 0, r)
        place(g, h, core, 0, r)

    def g2(g, h, j, r):
        wait(gat.at[g, h, core, back(0, h, j), back(1, h, r)], g2r.at[g, h, j - 1, r])
        if (g, r) not in LATE:
            hand_over(g, h, j, r)
        place(g, h, core, j, r)

    def last(g, h, j, r):
        wait(gat.at[g, h, 1 - core, back(0, h, j), back(1, h, r)], fr.at[g, h, j, r])
        place(g, h, 1 - core, j, r)

    def turn_back(h, zi, xi):
        parts = []
        for xj in (xi, xi + 1):
            for k in range(2):
                f, s = (xj, zi) if h == 0 else (zi, xj)
                parts.append(gat[1, h, k, f, s, 0])
        lane = pl.multiple_of((zi * 4 + xi) * 64, 128)
        cm[lanes_of(h), pl.ds(lane, 128)] = jnp.concatenate(parts, axis=0).T

    def finish(g, r):
        for j in (0, *BACK):
            for h in range(2):
                last(g, h, j, r)
        if g == 1:
            for xi in (0, 2):
                turn_back(0, back(1, 0, r), xi)

    def n1():
        wait(npair, nr.at[0])
        nx[x] = nbuf[...] + npair[...]
        for j in (2, 1, 3):
            remote(nx.at[x], nx.at[x], ns.at[1], nr.at[1], ahead(0, j))

    def n2():
        wait(nx.at[pl.ds(0, 3)], nr.at[1])
        nz[z] = ((nx[0] + nx[1]) + nx[2]) + nx[3]
        for j in (2, 1, 3):
            remote(nz.at[z], nz.at[z], ns.at[2], nr.at[2], ahead(1, j))

    def n3():
        wait(nz.at[pl.ds(0, 3)], nr.at[2])
        new = ((nz[0] + nz[1]) + nz[2]) + nz[3]
        cn[...] = new[0].astype(BF16)
        cb[...] = new[1].astype(BF16)
        place = jnp.sum(jnp.where(mine[None], new, 0.0), axis=1)
        slot = ((place[:, 0:32] + place[:, 32:64]) + place[:, 64:96]) + place[:, 96:128]
        sn[...] = slot[0:1]
        sb[...] = slot[1:2]

    both = range(2)

    def over(stage, g, *choices):
        for c in choices:
            for h in both:
                stage(g, h, *(c if isinstance(c, tuple) else (c,)))

    def gathered(g):
        before = None
        for r in (0, *BACK):
            over(g2, g, *((j, r) for j in BACK))
            if before is not None:
                finish(g, before)
            before = r

    @pl.when(core == 1)
    def _():
        pl.semaphore_wait(barrier, 6)
        pl.semaphore_signal(hands, inc=1, device_id=partner, device_id_type=MESH)

    @pl.when(core == 0)
    def _():
        pl.semaphore_wait(hands, 1)

    over(e1, 0, 2)
    over(e1, 0, 1)
    turned.wait()
    for c in range(4):
        turn(c)
    value.wait()
    over(share, 1, *ORDER)
    over(e1, 0, 3, 0)
    over(e1, 1, *ORDER)
    n1()
    over(r1, 0, *ORDER)
    for copy in masters:
        copy.wait()
    over(r1, 1, 2, 1, 3)
    over(r2, 0, ())
    over(own, 0, ())
    over(r1, 1, 0)
    n2()
    over(r2, 1, ())
    over(own, 1, ())
    over(g1, 0, 1, 3, 2)
    over(g1, 1, 1, 3, 2)
    n3()
    gathered(0)
    over(g2, 1, *((j, 0) for j in BACK))
    over(g2, 1, *((j, 1) for j in BACK))
    finish(1, 0)
    finish(0, 2)
    over(g2, 1, *((j, 3) for j in BACK))
    finish(1, 1)
    over(g2, 1, *((j, 2) for j in BACK))
    finish(1, 3)
    for zi in range(4):
        turn_back(1, zi, x // 2 * 2)
    for i, ref in enumerate((pair, send1, send2, send2, send1)):
        wait(ref, sent.at[i])
    wait(nbuf, ns.at[0])
    wait(nx.at[pl.ds(0, 3)], ns.at[1])
    wait(nz.at[pl.ds(0, 3)], ns.at[2])
    finish(1, 2)
    for zi in range(4):
        turn_back(1, zi, 2 - x // 2 * 2)
    wait(gat.at[:, 0], sent.at[5])


def placed(*refs):
    sems = refs[24]
    copies = [pltpu.make_async_copy(refs[i], refs[12 + i], sems.at[i]) for i in range(12)]
    for copy in copies:
        copy.start()
    for copy in copies:
        copy.wait()


def per_device(pq, pk, pv, pm, pn, pb, mq, mk, mv, mm, mn, mb):
    blocks = (4, 4, 2, 32, 256)
    hbm = pl.BlockSpec(memory_space=pl.ANY)
    vmem = pl.BlockSpec(memory_space=pltpu.VMEM)
    dma = pltpu.SemaphoreType.DMA
    gathered = jax.ShapeDtypeStruct((4, 4, 2, 32, 256), BF16)
    share = jax.ShapeDtypeStruct((32, 256), F32)
    small = jax.ShapeDtypeStruct((8, 128), BF16)
    slot = jax.ShapeDtypeStruct((1, 32), F32)
    shapes = (jax.ShapeDtypeStruct((256, 1024), BF16), gathered, gathered, gathered, small, small)
    shapes += (share,) * 4 + (slot,) * 2
    out = pl.pallas_call(
        kernel,
        out_shape=tuple(pltpu.VMEM(o.shape, o.dtype) for o in shapes),
        in_specs=[hbm] * 12,
        out_specs=(vmem,) * 12,
        scratch_shapes=[
            pltpu.VMEM((2, 2, *blocks), F32),
            pltpu.VMEM((256, 1024), F32),
            pltpu.VMEM((2, 2, 4, 2, 4, 32, 128), F32),
            pltpu.VMEM((2, 2, 4, 3, 2, 32, 128), BF16),
            pltpu.VMEM((2, 2, 4, 3, 2, 32, 128), BF16),
            pltpu.VMEM((2, 2, 3, 2, 32, 128), BF16),
            pltpu.VMEM((2, 2, 3, 2, 32, 128), BF16),
            pltpu.VMEM((2, 2, 2, 32, 128), F32),
            pltpu.VMEM((2, 2, 2, 4, 4, 2, 32, 128), BF16),
            pltpu.VMEM((4, 32, 256), F32),
            pltpu.VMEM((2, 8, 128), F32),
            pltpu.VMEM((2, 8, 128), F32),
            pltpu.VMEM((4, 2, 8, 128), F32),
            pltpu.VMEM((4, 2, 8, 128), F32),
            pltpu.VMEM((2, 1, 32), F32),
            dma((2, 4, 2)),
            dma((6,)),
            dma((4,)),
            dma((2, 2, 4)),
            dma((2, 2, 4)),
            dma((2, 2)),
            dma((2, 2, 3)),
            dma((2, 2, 3, 4)),
            dma((2, 2, 4, 4)),
            dma((6,)),
            dma((3,)),
            dma((3,)),
            pltpu.SemaphoreType.REGULAR,
        ],
        compiler_params=pltpu.CompilerParams(collective_id=0, has_side_effects=True, vmem_limit_bytes=60 * 2**20),
        name="step",
    )(
        pm[0], pq.reshape(blocks), pk.reshape(blocks), pv.reshape(blocks), pn.reshape(8, 128), pb.reshape(8, 128),
        mm.T, mq, mk, mv, mn.reshape(1, 32), mb.reshape(1, 32),
    )
    cm, cq, ck, cv, cn, cb, sm, sq, sk, sv, sn, sb = pl.pallas_call(
        placed,
        out_shape=shapes,
        in_specs=[vmem] * 12,
        out_specs=(hbm,) * 12,
        scratch_shapes=[dma((12,))],
        name="placed",
    )(*[pltpu.with_memory_space_constraint(o, pltpu.VMEM) for o in out])
    whole = (1024, 256)
    return (
        cq.reshape(whole), ck.reshape(whole), cv.reshape(whole), cm, cn.reshape(1024), cb.reshape(1024),
        sq, sk, sv, sm.T, sn.reshape(32), sb.reshape(32),
    )


def solution(mesh):
    in_specs = (
        P("batch", None, "cols"),
        P("batch", None, "cols"),
        P("batch", None, "cols"),
        P("batch", "cols", None),
        P("batch", None),
        P("batch", None),
        P("batch", "cols"),
        P("batch", "cols"),
        P("batch", "cols"),
        P("cols", "batch"),
        P("batch"),
        P("batch"),
    )
    out_specs = (
        P(None, "cols"),
        P(None, "cols"),
        P(None, "cols"),
        P("cols", None),
        P(),
        P(),
        P("batch", "cols"),
        P("batch", "cols"),
        P("batch", "cols"),
        P("cols", "batch"),
        P("batch"),
        P("batch"),
    )
    return jax.shard_map(per_device, mesh=mesh, in_specs=in_specs, out_specs=out_specs, check_vma=False)
```

```python
import math

import jax
import jax.numpy as jnp
from jax import lax
from jax.experimental import pallas as pl
from jax.experimental.pallas import tpu as pltpu
from jax.sharding import PartitionSpec as P

MESH = pl.DeviceIdType.MESH
F32 = jnp.float32
BF16 = jnp.bfloat16

RATE = 0.4 * 32**-0.5

SPREAD = 15.75
STEPS = 65536.0
SHIFT = 125.0
PAIR_TOP = 2.6
ORDER = (2, 1, 3, 0)
LATE = ((1, 2), (1, 3))
BACK = (1, 3, 2)
FOUR_TOP = 10.4


def encoded(x, top):
    log = jnp.log(1.0 + jnp.abs(x) * (STEPS / top))
    v = jnp.exp2(log * (SPREAD / math.log(2.0)) - SHIFT)
    return jnp.where(x < 0, -v, v).astype(BF16)


def decoded(code, top):
    v = code.astype(F32)
    log = jnp.log(jnp.abs(v))
    size = (jnp.exp2(log * (1.0 / (SPREAD * math.log(2.0))) + SHIFT / SPREAD) - 1.0) * (top / STEPS)
    return jnp.where(v < 0, -size, size)


def kernel(
    pm, pq, pk, pv, pn, pb, mm, mq, mk, mv, mn, mb,
    cm, cq, ck, cv, cn, cb, sm, sq, sk, sv, sn, sb,
    raw, flat, pair, send1, recv1, send2, recv2, acc, gat, mast,
    nbuf, npair, nx, nz, nmast,
    load_sem, mload_sem, nload_sem, d_recv, s1r, s2r, g1r, g2r, fr, sent, ns, nr, hands,
):
    b = lax.axis_index("batch")
    col = lax.axis_index("cols")
    z, x, core = b // 8, (b // 2) % 4, b % 2
    first, second = (x, z), (z, x)

    def at(z, x, core):
        return (z * 8 + x * 2 + core, col)

    def ahead(axis, j, core=core):
        return at(z, (x + j) % 4, core) if axis == 0 else at((z + j) % 4, x, core)

    def wait(ref, sem):
        pltpu.make_async_copy(ref, ref, sem).wait()

    def remote(src, dst, ssem, rsem, dev):
        pltpu.make_async_remote_copy(
            src_ref=src, dst_ref=dst, send_sem=ssem, recv_sem=rsem, device_id=dev, device_id_type=MESH
        ).start()

    def lanes_of(h):
        return slice(128 * h, 128 * h + 128)

    def piece(ref, h, k, core=None):
        cores = slice(None) if core is None else core
        return ref.at[k, :, cores, :, lanes_of(h)] if h == 0 else ref.at[:, k, cores, :, lanes_of(h)]

    def pieces(g, h, k, core):
        ref = raw.at[g]
        return ref.at[:, k, :, core, :, lanes_of(h)] if h == 0 else ref.at[:, :, k, core, :, lanes_of(h)]

    barrier = pltpu.get_barrier_semaphore()
    partner = at(z, x, 1 - core)
    far = [ahead(axis, j) for j in (2, 1, 3) for axis in (0, 1)]

    @pl.when(core == 1)
    def _():
        pl.semaphore_signal(barrier, inc=1, device_id=partner, device_id_type=MESH)

    turned = pltpu.make_async_copy(pm, flat, mload_sem.at[4])
    loads = {
        (h, r, i): pltpu.make_async_copy(
            piece(ref, h, (second[h] + r) % 4), piece(raw.at[0, i], h, (second[h] + r) % 4), load_sem.at[h, r, i]
        )
        for r in ORDER
        for h in range(2)
        for i, ref in enumerate((pq, pk))
    }
    value = pltpu.make_async_copy(pv, raw.at[1, 1], mload_sem.at[5])
    small = [
        pltpu.make_async_copy(pn, nbuf.at[0], nload_sem.at[0]),
        pltpu.make_async_copy(pb, nbuf.at[1], nload_sem.at[1]),
        pltpu.make_async_copy(mn, nmast.at[0], nload_sem.at[2]),
        pltpu.make_async_copy(mb, nmast.at[1], nload_sem.at[3]),
    ]
    masters = [pltpu.make_async_copy(ref, mast.at[a], mload_sem.at[a]) for a, ref in enumerate((mq, mk, mm, mv))]
    for copy in (*loads.values(), *small, turned, value, *masters):
        copy.start()

    def share(g, h, r):
        k = (second[h] + r) % 4
        remote(pieces(g, h, k, 1 - core), pair.at[g, h, k], sent.at[0], d_recv.at[g, h, r], partner)

    @pl.when(core == 0)
    def _():
        pl.semaphore_wait(barrier, 1)
        pl.semaphore_signal(hands, inc=1, device_id=partner, device_id_type=MESH)

    @pl.when(core == 1)
    def _():
        pl.semaphore_wait(hands, 1)
        for peer in far:
            pl.semaphore_signal(barrier, inc=1, device_id=peer, device_id_type=MESH)

    for r in ORDER:
        for h in range(2):
            for i in range(2):
                loads[h, r, i].wait()
            share(0, h, r)

    def turn(c):
        raw[1, 0, c] = flat[:, 256 * c : 256 * c + 256].T.reshape(4, 2, 32, 256)

    def block(g, i, h, f, k):
        zi, xi = (k, f) if h == 0 else (f, k)
        return raw[g, i, zi, xi, core, :, lanes_of(h)] + pair[g, h, k, i, f]

    def e1(g, h, r):
        k = (second[h] + r) % 4
        wait(pair.at[g, h, k], d_recv.at[g, h, r])
        for j in (2, 1, 3):
            for i in range(2):
                send1[g, h, r, j - 1, i] = encoded(block(g, i, h, (first[h] + j) % 4, k), PAIR_TOP)
            remote(send1.at[g, h, r, j - 1], recv1.at[g, h, r, j - 1], sent.at[1], s1r.at[g, h, r], ahead(h, j))

    def r1(g, h, r):
        k = (second[h] + r) % 4
        wait(recv1.at[g, h, r], s1r.at[g, h, r])
        for i in range(2):
            t = block(g, i, h, first[h], k)
            for j in range(3):
                t += decoded(recv1[g, h, r, j, i], PAIR_TOP)
            if r:
                send2[g, h, r - 1, i] = encoded(t, FOUR_TOP)
            else:
                acc[g, h, i] = t
        if r:
            remote(send2.at[g, h, r - 1], recv2.at[g, h, r - 1], sent.at[2], s2r.at[g, h], ahead(1 - h, r))

    stepped = (sq, sk, sm, sv)

    def r2(g, h):
        wait(recv2.at[g, h], s2r.at[g, h])
        for i in range(2):
            t = acc[g, h, i]
            for j in range(3):
                t += decoded(recv2[g, h, j, i], FOUR_TOP)
            new = mast[2 * g + i, :, lanes_of(h)] - RATE * t
            stepped[2 * g + i][:, lanes_of(h)] = new
            gat[g, h, core, first[h], second[h], i] = new.astype(BF16)
        part = gat.at[g, h, core, first[h], second[h]]
        for j in (2, 1, 3):
            remote(part, part, sent.at[3], g1r.at[g, h, j - 1], ahead(1 - h, j))

    def back(axis, h, j):
        return ((first, second)[axis][h] + 4 - j) % 4

    def spread(g, h, r):
        part = gat.at[g, h, core, first[h], back(1, h, r)]
        for j in (2, 1, 3):
            remote(part, part, sent.at[4], g2r.at[g, h, j - 1, r], ahead(h, j))
        for j in (2, 1, 3) if (g, r) in LATE else ():
            remote(part, part, sent.at[5], fr.at[g, h, j, r], ahead(h, j, 1 - core))

    def hand_over(g, h, j, r):
        part = gat.at[g, h, core, back(0, h, j), back(1, h, r)]
        remote(part, part, sent.at[5], fr.at[g, h, j, r], partner)

    outs = (cq, ck, cm, cv)

    def place(g, h, k, j, r):
        f, s = back(0, h, j), back(1, h, r)
        zi, xi = (s, f) if h == 0 else (f, s)
        for i in range(2):
            if 2 * g + i != 2:
                outs[2 * g + i][zi, xi, k, :, lanes_of(h)] = gat[g, h, k, f, s, i]

    def own(g, h):
        spread(g, h, 0)
        hand_over(g, h, 0, 0)
        place(g, h, core, 0, 0)

    def g1(g, h, r):
        wait(gat.at[g, h, core, first[h], back(1, h, r)], g1r.at[g, h, r - 1])
        spread(g, h, r)
        hand_over(g, h, 0, r)
        place(g, h, core, 0, r)

    def g2(g, h, j, r):
        wait(gat.at[g, h, core, back(0, h, j), back(1, h, r)], g2r.at[g, h, j - 1, r])
        if (g, r) not in LATE:
            hand_over(g, h, j, r)
        place(g, h, core, j, r)

    def last(g, h, j, r):
        wait(gat.at[g, h, 1 - core, back(0, h, j), back(1, h, r)], fr.at[g, h, j, r])
        place(g, h, 1 - core, j, r)

    def turn_back(h, zi, xi):
        parts = []
        for xj in (xi, xi + 1):
            for k in range(2):
                f, s = (xj, zi) if h == 0 else (zi, xj)
                parts.append(gat[1, h, k, f, s, 0])
        lane = pl.multiple_of((zi * 4 + xi) * 64, 128)
        cm[lanes_of(h), pl.ds(lane, 128)] = jnp.concatenate(parts, axis=0).T

    def finish(g, r):
        for j in (0, *BACK):
            for h in range(2):
                last(g, h, j, r)
        if g == 1:
            for xi in (0, 2):
                turn_back(0, back(1, 0, r), xi)

    def n1():
        wait(npair, nr.at[0])
        nx[x] = nbuf[...] + npair[...]
        for j in (2, 1, 3):
            remote(nx.at[x], nx.at[x], ns.at[1], nr.at[1], ahead(0, j))

    def n2():
        wait(nx.at[pl.ds(0, 3)], nr.at[1])
        nz[z] = ((nx[0] + nx[1]) + nx[2]) + nx[3]
        for j in (2, 1, 3):
            remote(nz.at[z], nz.at[z], ns.at[2], nr.at[2], ahead(1, j))

    def n3():
        wait(nz.at[pl.ds(0, 3)], nr.at[2])
        new = ((nz[0] + nz[1]) + nz[2]) + nz[3]
        cn[...] = new[0].astype(BF16)
        cb[...] = new[1].astype(BF16)
        place = jnp.sum(jnp.where(mine[None], new, 0.0), axis=1)
        slot = ((place[:, 0:32] + place[:, 32:64]) + place[:, 64:96]) + place[:, 96:128]
        sn[...] = slot[0:1]
        sb[...] = slot[1:2]

    both = range(2)

    def over(stage, g, *choices):
        for c in choices:
            for h in both:
                stage(g, h, *(c if isinstance(c, tuple) else (c,)))

    def gathered(g):
        before = None
        for r in (0, *BACK):
            over(g2, g, *((j, r) for j in BACK))
            if before is not None:
                finish(g, before)
            before = r

    @pl.when(core == 1)
    def _():
        pl.semaphore_wait(barrier, 6)
        pl.semaphore_signal(hands, inc=1, device_id=partner, device_id_type=MESH)

    @pl.when(core == 0)
    def _():
        pl.semaphore_wait(hands, 1)

    over(e1, 0, 2)
    for copy in small:
        copy.wait()
    lanes = lax.broadcasted_iota(jnp.int32, (8, 128), 1)
    rows = lax.broadcasted_iota(jnp.int32, (8, 128), 0)
    mine = (rows * 4 + lanes // 32) == b
    for i in range(2):
        m = jnp.concatenate([nmast[i]] * 4, axis=1)
        nbuf[i] = jnp.where(mine, jnp.broadcast_to(m, (8, 128)), 0.0) - RATE * nbuf[i]
    remote(nbuf, npair, ns.at[0], nr.at[0], partner)
    over(e1, 0, 1)
    turned.wait()
    for c in range(4):
        turn(c)
    value.wait()
    over(share, 1, *ORDER)
    over(e1, 0, 3, 0)
    over(e1, 1, *ORDER)
    n1()
    over(r1, 0, *ORDER)
    for copy in masters:
        copy.wait()
    over(r1, 1, 2, 1, 3)
    over(r2, 0, ())
    over(own, 0, ())
    over(r1, 1, 0)
    n2()
    over(r2, 1, ())
    over(own, 1, ())
    over(g1, 0, 1, 3, 2)
    over(g1, 1, 1, 3, 2)
    n3()
    gathered(0)
    over(g2, 1, *((j, 0) for j in BACK))
    over(g2, 1, *((j, 1) for j in BACK))
    finish(1, 0)
    finish(0, 2)
    over(g2, 1, *((j, 3) for j in BACK))
    finish(1, 1)
    over(g2, 1, *((j, 2) for j in BACK))
    finish(1, 3)
    for zi in range(4):
        turn_back(1, zi, x // 2 * 2)
    for i, ref in enumerate((pair, send1, send2, send2, send1)):
        wait(ref, sent.at[i])
    wait(nbuf, ns.at[0])
    wait(nx.at[pl.ds(0, 3)], ns.at[1])
    wait(nz.at[pl.ds(0, 3)], ns.at[2])
    finish(1, 2)
    for zi in range(4):
        turn_back(1, zi, 2 - x // 2 * 2)
    wait(gat.at[:, 0], sent.at[5])


def placed(*refs):
    sems = refs[24]
    copies = [pltpu.make_async_copy(refs[i], refs[12 + i], sems.at[i]) for i in range(12)]
    for copy in copies:
        copy.start()
    for copy in copies:
        copy.wait()


def per_device(pq, pk, pv, pm, pn, pb, mq, mk, mv, mm, mn, mb):
    blocks = (4, 4, 2, 32, 256)
    hbm = pl.BlockSpec(memory_space=pl.ANY)
    vmem = pl.BlockSpec(memory_space=pltpu.VMEM)
    dma = pltpu.SemaphoreType.DMA
    gathered = jax.ShapeDtypeStruct((4, 4, 2, 32, 256), BF16)
    share = jax.ShapeDtypeStruct((32, 256), F32)
    small = jax.ShapeDtypeStruct((8, 128), BF16)
    slot = jax.ShapeDtypeStruct((1, 32), F32)
    shapes = (jax.ShapeDtypeStruct((256, 1024), BF16), gathered, gathered, gathered, small, small)
    shapes += (share,) * 4 + (slot,) * 2
    out = pl.pallas_call(
        kernel,
        out_shape=tuple(pltpu.VMEM(o.shape, o.dtype) for o in shapes),
        in_specs=[hbm] * 12,
        out_specs=(vmem,) * 12,
        scratch_shapes=[
            pltpu.VMEM((2, 2, *blocks), F32),
            pltpu.VMEM((256, 1024), F32),
            pltpu.VMEM((2, 2, 4, 2, 4, 32, 128), F32),
            pltpu.VMEM((2, 2, 4, 3, 2, 32, 128), BF16),
            pltpu.VMEM((2, 2, 4, 3, 2, 32, 128), BF16),
            pltpu.VMEM((2, 2, 3, 2, 32, 128), BF16),
            pltpu.VMEM((2, 2, 3, 2, 32, 128), BF16),
            pltpu.VMEM((2, 2, 2, 32, 128), F32),
            pltpu.VMEM((2, 2, 2, 4, 4, 2, 32, 128), BF16),
            pltpu.VMEM((4, 32, 256), F32),
            pltpu.VMEM((2, 8, 128), F32),
            pltpu.VMEM((2, 8, 128), F32),
            pltpu.VMEM((4, 2, 8, 128), F32),
            pltpu.VMEM((4, 2, 8, 128), F32),
            pltpu.VMEM((2, 1, 32), F32),
            dma((2, 4, 2)),
            dma((6,)),
            dma((4,)),
            dma((2, 2, 4)),
            dma((2, 2, 4)),
            dma((2, 2)),
            dma((2, 2, 3)),
            dma((2, 2, 3, 4)),
            dma((2, 2, 4, 4)),
            dma((6,)),
            dma((3,)),
            dma((3,)),
            pltpu.SemaphoreType.REGULAR,
        ],
        compiler_params=pltpu.CompilerParams(collective_id=0, has_side_effects=True, vmem_limit_bytes=60 * 2**20),
        name="step",
    )(
        pm[0], pq.reshape(blocks), pk.reshape(blocks), pv.reshape(blocks), pn.reshape(8, 128), pb.reshape(8, 128),
        mm.T, mq, mk, mv, mn.reshape(1, 32), mb.reshape(1, 32),
    )
    cm, cq, ck, cv, cn, cb, sm, sq, sk, sv, sn, sb = pl.pallas_call(
        placed,
        out_shape=shapes,
        in_specs=[vmem] * 12,
        out_specs=(hbm,) * 12,
        scratch_shapes=[dma((12,))],
        name="placed",
    )(*[pltpu.with_memory_space_constraint(o, pltpu.VMEM) for o in out])
    whole = (1024, 256)
    return (
        cq.reshape(whole), ck.reshape(whole), cv.reshape(whole), cm, cn.reshape(1024), cb.reshape(1024),
        sq, sk, sv, sm.T, sn.reshape(32), sb.reshape(32),
    )


def solution(mesh):
    in_specs = (
        P("batch", None, "cols"),
        P("batch", None, "cols"),
        P("batch", None, "cols"),
        P("batch", "cols", None),
        P("batch", None),
        P("batch", None),
        P("batch", "cols"),
        P("batch", "cols"),
        P("batch", "cols"),
        P("cols", "batch"),
        P("batch"),
        P("batch"),
    )
    out_specs = (
        P(None, "cols"),
        P(None, "cols"),
        P(None, "cols"),
        P("cols", None),
        P(),
        P(),
        P("batch", "cols"),
        P("batch", "cols"),
        P("batch", "cols"),
        P("cols", "batch"),
        P("batch"),
        P("batch"),
    )
    return jax.shard_map(per_device, mesh=mesh, in_specs=in_specs, out_specs=out_specs, check_vma=False)
```
